256 devices in a mesh: dom: 32 (over y, x, core), col: 8 (over z).
Axes of the slice: x: 4, y: 4, z: 8, core: 2. Of those that a mesh axis runs over, the one named last changes fastest.
Arguments:
- features: bfloat16 [262144, 1024], P('dom', 'col'), may hold values from -6 to 6
- requests: int32 [32, 32, 8], P('dom'), may hold values from 0 to 63
- counts: int32 [32, 32], P(None, 'dom'), may hold values from 0 to 8, as said below
- tile_block: int32 [512, 32], P('dom'), may hold values from 0 to 127
- local_nbr: int32 [65536, 128], P('dom'), may hold values from 0 to 127
- tile_count: int32 [512], P('dom'), may hold values from 1 to 32, as said below
- w_self: bfloat16 [1024, 1024], P('col'), may hold values from -0.125 to 0.125
- w_neigh: bfloat16 [1024, 1024], P('col'), may hold values from -0.75 to 0.75
Outputs:
- embeddings: bfloat16 [65536, 1024], P('dom', 'col')
The draws below stay inside these ranges and needn't reach their ends.
Inputs may be any that keep to these rules, and one draw needn't show every extreme that they name: Each shard's counts over all partitions sum to 128; for every shard some partition has exactly 8. `tile_count`: on every shard some destination block uses all 32 tiles.
All inputs are finite; a program needn't handle non-finite values.
Results may differ from the reference program's by a relative error of at most 0.014.
Values may be sent and summed in bfloat16 or wider, within the bound.
No kernel may reach another device: no remote copies, remote signals or barrier semaphores. Data moves between devices by JAX's collectives and lax.ppermute only.
A program may use at most 128 MiB of HBM per device.

```python
import jax
import jax.numpy as jnp
from jax import lax

D = 1024
BLOCK_ROWS = 128
BLK_DEV = 64
CAP = 8
DST_BLK = 16
TILES = 32
FAN_T = 4
FRONT = 128
BLOCKS = 2048
DST_BLOCKS = 512
COL_W = 128
N_DOM = 32


def draw_counts(key, part):
    key_order, key_share, key_heat = jax.random.split(key, 3)
    heat = jax.random.permutation(key_heat, N_DOM)
    orders = jax.vmap(lambda subkey: jax.random.permutation(subkey, N_DOM))(jax.random.split(key_order, N_DOM))
    share = jax.random.randint(key_share, (N_DOM, N_DOM // 2), 0, CAP + 1)
    share = share.at[:, 0].set(CAP)
    first_half = orders[:, 0::2]
    second_half = orders[:, 1::2]
    larger = jnp.maximum(share, CAP - share)
    hotter = heat[first_half] > heat[second_half]
    first_count = jnp.where(hotter, larger, CAP - larger)
    second_count = CAP - first_count
    shard_rows = jnp.arange(N_DOM)[:, None]
    grid = jnp.zeros((N_DOM, N_DOM), jnp.int32)
    grid = grid.at[shard_rows, first_half].set(first_count)
    grid = grid.at[shard_rows, second_half].set(second_count)
    return grid.T.astype(jnp.int32)


def draw_tile_count(key, part):
    key_level, key_raw, key_where = jax.random.split(key, 3)
    levels = jax.random.randint(key_level, (N_DOM, 1), TILES // 4, TILES + 1)
    raw_bits = jax.random.randint(key_raw, (N_DOM, DST_BLK), 0, 1 << 20)
    result = 1 + raw_bits % levels
    full_at = jax.random.randint(key_where, (N_DOM, 1), 0, DST_BLK)
    result = jnp.where(jnp.arange(DST_BLK)[None, :] == full_at, TILES, result)
    return result.reshape(-1).astype(jnp.int32)


def place_ends(drawn, own_key, low, high):
    index_at = [jax.random.randint(jax.random.fold_in(own_key, axis), (), 0, length) for axis, length in enumerate(drawn.shape)]
    main_axis = drawn.shape.index(max(drawn.shape))
    neighbour = index_at[:main_axis] + [(index_at[main_axis] + 1) % drawn.shape[main_axis]] + index_at[main_axis + 1:]
    return drawn.at[tuple(index_at)].set(low).at[tuple(neighbour)].set(high)


def level_of(rng, dims, cuts, low, top_value):
    loudness, own = 1.0, jax.random.fold_in(rng, 6)
    for position, shards_of in cuts:
        heights = jnp.exp(jax.random.uniform(jax.random.fold_in(own, position), (shards_of,), jnp.float32, low / len(cuts), top_value / len(cuts)))
        loudness = loudness * jnp.repeat(heights, dims[position] // shards_of).reshape([-1 if axis == position else 1 for axis in range(len(dims))])
    return loudness


def gaussian(rng, extent, spread, bound, cuts=(), kind=jnp.bfloat16):
    entries = jax.random.normal(rng, extent, jnp.float32) * spread
    if len(cuts) > 0:
        entries = level_of(rng, extent, cuts, -0.22, 0.18) * entries
    return jnp.clip(entries, min=-bound, max=bound).astype(kind)


def setup_inputs(seed: int = 0) -> dict:
    seeds = jax.random.split(jax.random.key(seed), 9)
    return {
        "features": gaussian(seeds[0], (BLOCKS * BLOCK_ROWS, D), 1.0, 6.0, ((0, 32), (1, 8))),
        "requests": place_ends(jax.random.randint(seeds[1], (N_DOM, N_DOM, CAP), 0, BLK_DEV), jax.random.fold_in(seeds[1], 1), 0, BLK_DEV - 1).astype(jnp.int32),
        "counts": draw_counts(jax.random.fold_in(seeds[8], 71), 0),
        "tile_block": place_ends(jax.random.randint(seeds[3], (DST_BLOCKS, TILES), 0, FRONT), jax.random.fold_in(seeds[3], 1), 0, FRONT - 1).astype(jnp.int32),
        "local_nbr": place_ends(jax.random.randint(seeds[4], (DST_BLOCKS * BLOCK_ROWS, TILES * FAN_T), 0, BLOCK_ROWS), jax.random.fold_in(seeds[4], 1), 0, BLOCK_ROWS - 1).astype(jnp.int32),
        "tile_count": draw_tile_count(jax.random.fold_in(seeds[8], 71), 0),
        "w_self": gaussian(seeds[6], (D, D), (2 * D) ** -0.5, 0.125, ((0, 8),)),
        "w_neigh": gaussian(seeds[7], (D, D), (D // 16) ** -0.5, 0.75, ((0, 8),)),
    }


def frontier_blocks(requests, counts):
    slot_ends = jnp.cumsum(counts, axis=0)
    slot_starts = slot_ends - counts
    positions = jnp.arange(FRONT, dtype=jnp.int32)

    def one_shard(ends_col, starts_col, wanted):
        owner_of = lax.optimization_barrier(jnp.sum((ends_col[None, :] <= positions[:, None]).astype(jnp.int32), axis=1))
        slot_pos = positions - starts_col[owner_of]
        return (owner_of * BLK_DEV + wanted[owner_of, slot_pos]).astype(jnp.int32)
    return jax.vmap(one_shard, in_axes=(1, 1, 1))(slot_ends, slot_starts, requests)

def reference(features, requests, counts, tile_block, local_nbr, tile_count, w_self, w_neigh):
    global_block = frontier_blocks(requests, counts)
    tile_ids = jnp.arange(TILES, dtype=jnp.int32)
    row_ids = jnp.arange(BLOCK_ROWS, dtype=jnp.int32)
    groups = D // COL_W
    self_mat = w_self.astype(jnp.float32).reshape(groups, COL_W, D)
    neigh_mat = w_neigh.astype(jnp.float32).reshape(groups, COL_W, D)

    def one_block(inputs):
        block_id, picks, neighbor, used_tiles = inputs
        shard_row = global_block[block_id // DST_BLK]
        tile_global = shard_row[picks]
        rows = tile_global[None, :, None] * BLOCK_ROWS + neighbor.reshape(BLOCK_ROWS, TILES, FAN_T)
        values = features[rows.reshape(-1)].astype(jnp.float32).reshape(BLOCK_ROWS, TILES, FAN_T, D)
        live_mask = (tile_ids < used_tiles).astype(jnp.float32)
        summed = lax.optimization_barrier(jnp.sum(values * live_mask[None, :, None, None], axis=(1, 2)))
        agg = (summed / (FAN_T * used_tiles).astype(jnp.float32)).astype(jnp.bfloat16)
        own = features[shard_row[block_id % DST_BLK] * BLOCK_ROWS + row_ids]
        pieces = jnp.einsum('rkc,kcj->krj', own.astype(jnp.float32).reshape(BLOCK_ROWS, groups, COL_W), self_mat, precision=lax.Precision.HIGHEST)
        pieces = pieces + jnp.einsum('rkc,kcj->krj', agg.astype(jnp.float32).reshape(BLOCK_ROWS, groups, COL_W), neigh_mat, precision=lax.Precision.HIGHEST)
        pieces = lax.optimization_barrier(pieces.astype(jnp.bfloat16)).astype(jnp.float32)
        hidden = jnp.maximum(lax.optimization_barrier(jnp.sum(pieces, axis=0)), 0.0)
        scale = jnp.sqrt(0.25 + lax.optimization_barrier(jnp.sum(hidden * hidden, axis=1, keepdims=True)) / D)
        return (hidden / scale).astype(jnp.bfloat16)
    block_ids = jnp.arange(DST_BLOCKS, dtype=jnp.int32)
    result = lax.map(one_block, (block_ids, tile_block, local_nbr.reshape(DST_BLOCKS, BLOCK_ROWS, TILES * FAN_T), tile_count))
    return result.reshape(DST_BLOCKS * BLOCK_ROWS, D)
```

```python
import functools

import jax
import jax.numpy as jnp
from jax import lax
from jax.experimental import pallas as pl
from jax.experimental.pallas import tpu as pltpu
from jax.sharding import PartitionSpec as P

D = 1024
ROWS = 128
CAP = 8
TILES = 32
FAN_T = 4
FRONT = 128
BF = jnp.bfloat16
F32 = jnp.float32
I32 = jnp.int32

VMEM = pl.BlockSpec(memory_space=pltpu.VMEM)
SMEM = pl.BlockSpec(memory_space=pltpu.SMEM)
ANY = pl.BlockSpec(memory_space=pl.ANY)


def prep_kernel(req, cnt, feat, nbr, ws, wn, packed, slot_of, nbr_t, w_t, ft, sem):
    n_blk = feat.shape[0] // ROWS
    n_req = packed.shape[0]

    def turn(b, _):
        ft[b] = feat[pl.ds(b * ROWS, ROWS), :].T
        return 0

    lax.fori_loop(0, n_blk, turn, 0)

    def send(q, _):
        pltpu.make_async_copy(ft.at[req[q // CAP, q % CAP]], packed.at[q], sem).start()
        return 0

    lax.fori_loop(0, n_req, send, 0)

    def owner(o, p):
        def slot(s, p):
            slot_of[p] = o * CAP + s
            return p + 1

        return lax.fori_loop(0, cnt[o], slot, p)

    lax.fori_loop(0, cnt.shape[0], owner, jnp.int32(0))

    def turn_nbr(i, _):
        nbr_t[i] = nbr[pl.ds(i * ROWS, ROWS), :].T.astype(F32)
        return 0

    lax.fori_loop(0, nbr_t.shape[0], turn_nbr, 0)
    for j in range(D // ROWS):
        lanes = slice(j * ROWS, (j + 1) * ROWS)
        w_t[lanes, :ROWS] = ws[:, lanes].T
        w_t[lanes, ROWS:] = wn[:, lanes].T
    pltpu.make_async_copy(packed, packed, sem).wait()


def prep(features, requests, counts, local_nbr, w_self, w_neigh):
    n_req = requests.shape[0] * CAP
    n_dst = local_nbr.shape[0] // ROWS
    return pl.pallas_call(
        prep_kernel,
        out_shape=(
            jax.ShapeDtypeStruct((n_req, ROWS, ROWS), BF),
            jax.ShapeDtypeStruct((FRONT,), I32),
            jax.ShapeDtypeStruct((n_dst, ROWS, ROWS), F32),
            jax.ShapeDtypeStruct((D, 2 * ROWS), BF),
        ),
        in_specs=[SMEM, SMEM, VMEM, VMEM, VMEM, VMEM],
        out_specs=(ANY, SMEM, VMEM, VMEM),
        scratch_shapes=[
            pltpu.VMEM((features.shape[0] // ROWS, ROWS, ROWS), BF),
            pltpu.SemaphoreType.DMA,
        ],
        name="prep",
    )(requests, counts, features, local_nbr, w_self, w_neigh)


def agg_kernel(slot_of, tile_block, tile_count, arrived, nbr_t, out):
    iota = lax.broadcasted_iota(I32, (ROWS, ROWS), 0).astype(F32).astype(BF)
    one, zero = jnp.ones((), BF), jnp.zeros((), BF)

    def weights(i, t, dead):
        total = None
        for f in range(FAN_T):
            row = nbr_t[i, pl.ds(t * FAN_T + f, 1), :] + dead
            hit = jnp.where(iota == row.astype(BF), one, zero)
            total = hit if total is None else total + hit
        return total

    def block(i, _):
        used = tile_count[i]

        def pair(h, acc):
            t0 = 2 * h
            t1 = t0 + 1
            dead = jnp.where(t1 < used, 0.0, 512.0).astype(F32)
            left = arrived[slot_of[tile_block[i, t0]]]
            right = arrived[slot_of[tile_block[i, t1]]]
            onehot = jnp.concatenate([weights(i, t0, jnp.float32(0.0)), weights(i, t1, dead)], axis=0)
            return acc + jnp.dot(jnp.concatenate([left, right], axis=1), onehot, preferred_element_type=F32)

        acc = lax.fori_loop(0, (used + 1) // 2, pair, jnp.zeros((ROWS, ROWS), F32))
        out[i, 0] = arrived[slot_of[i]]
        out[i, 1] = (acc / (used * FAN_T).astype(F32)).astype(BF)
        return 0

    lax.fori_loop(0, out.shape[0], block, 0)


def aggregate(slot_of, tile_block, tile_count, arrived, nbr_t):
    n_dst = nbr_t.shape[0]
    return pl.pallas_call(
        agg_kernel,
        out_shape=jax.ShapeDtypeStruct((n_dst, 2, ROWS, ROWS), BF),
        in_specs=[SMEM, SMEM, SMEM, VMEM, VMEM],
        out_specs=VMEM,
        name="agg",
    )(slot_of, tile_block, tile_count, arrived, nbr_t)


def project_kernel(me, x, *refs):
    *w_t, out, hid = refs
    n_col = x.shape[0]
    for b in range(x.shape[1]):
        for n0 in range(0, D, 256):
            total = None
            for k in range(n_col):
                group = lax.rem(me[0] + n_col - k, n_col)
                part = jnp.dot(
                    w_t[k][n0 : n0 + 256, :], x[group, b].reshape(2 * ROWS, ROWS), preferred_element_type=F32
                )
                total = part if total is None else total + part
            hid[n0 : n0 + 256, :] = jnp.maximum(total, 0.0)
        h = hid[...]
        scale = jnp.sqrt(0.25 + jnp.sum(h * h, axis=0, keepdims=True) / D)
        for j in range(n_col):
            piece = hid[j * ROWS : (j + 1) * ROWS, :] / scale
            out[j, b * ROWS : (b + 1) * ROWS, :] = piece.T.astype(BF)


def project(me, x, w_t):
    n_col, n_blk = x.shape[:2]
    return pl.pallas_call(
        project_kernel,
        out_shape=jax.ShapeDtypeStruct((n_col, n_blk * ROWS, ROWS), BF),
        in_specs=[SMEM] + [VMEM] * (1 + n_col),
        out_specs=VMEM,
        scratch_shapes=[pltpu.VMEM((D, ROWS), F32)],
        name="project",
    )(me, x, *w_t)


def on_device(features, requests, counts, tile_block, local_nbr, tile_count, w_self, w_neigh):
    n_dom, n_col = lax.axis_size("dom"), lax.axis_size("col")
    packed, slot_of, nbr_t, w_t = prep(features, requests[0], counts[:, 0], local_nbr, w_self, w_neigh)
    me = lax.axis_index("col")
    w_all = [w_t]
    for k in range(1, n_col):
        w_all.append(lax.ppermute(w_t, "col", [(i, (i + k) % n_col) for i in range(n_col)]))
    arrived = lax.all_to_all(packed.reshape(n_dom, CAP, ROWS, ROWS), "dom", 0, 0, tiled=True)
    arrived = arrived.reshape(n_dom * CAP, ROWS, ROWS)
    x = aggregate(slot_of, tile_block, tile_count, arrived, nbr_t)
    n_dst = x.shape[0]
    x = lax.all_to_all(x.reshape(n_col, n_dst // n_col, 2, ROWS, ROWS), "col", 0, 0, tiled=True)
    y = project(me.reshape(1).astype(I32), x, w_all)
    y = lax.all_to_all(y, "col", 0, 0, tiled=True)
    return y.reshape(-1, ROWS)


def solution(mesh):
    return jax.shard_map(
        on_device,
        mesh=mesh,
        in_specs=(
            P("dom", "col"),
            P("dom", None, None),
            P(None, "dom"),
            P("dom", None),
            P("dom", None),
            P("dom"),
            P("col", None),
            P("col", None),
        ),
        out_specs=P("dom", "col"),
        check_vma=False,
    )
```

```python
import functools

import jax
import jax.numpy as jnp
from jax import lax
from jax.experimental import pallas as pl
from jax.experimental.pallas import tpu as pltpu
from jax.sharding import PartitionSpec as P

D = 1024
ROWS = 128
CAP = 8
TILES = 32
FAN_T = 4
FRONT = 128
RING = 4
N_SRC = 2 * RING
DST = 16
BUCKET = RING * DST * TILES + 8
UNROLL = 4
BF = jnp.bfloat16
F32 = jnp.float32
I32 = jnp.int32

VMEM = pl.BlockSpec(memory_space=pltpu.VMEM)
SMEM = pl.BlockSpec(memory_space=pltpu.SMEM)
ANY = pl.BlockSpec(memory_space=pl.ANY)


def dom_of(y, x, core):
    return (y * RING + x) * 2 + core


def meet_pairs(d, e):
    pairs = []
    for y in range(RING):
        for x in range(RING):
            for core in range(2):
                if core ^ e == 0:
                    pairs.append((dom_of(y, x, core), dom_of((y + d) % RING, x, 0)))
                else:
                    pairs.append((dom_of(y, x, core), dom_of(y, (x + d) % RING, 1)))
    return pairs


def ring_pairs(m):
    pairs = []
    for y in range(RING):
        for x in range(RING):
            pairs.append((dom_of(y, x, 0), dom_of(y, (x + m) % RING, 0)))
            pairs.append((dom_of(y, x, 1), dom_of((y + m) % RING, x, 1)))
    return pairs


def wrapped(v):
    return lax.rem(v + 2 * RING, RING)


def pack_kernel(me, req, feat, *refs):
    outs, (ft, stage, sem) = refs[:N_SRC], refs[N_SRC:]
    core, x, y = lax.rem(me[0], 2), lax.rem(me[0] // 2, RING), me[0] // (2 * RING)

    def turn(b, _):
        for u in range(8):
            ft[b * 8 + u] = feat[pl.ds((b * 8 + u) * ROWS, ROWS), :].T
        return 0

    lax.fori_loop(0, feat.shape[0] // ROWS // 8, turn, 0)
    copies = []
    for q in range(N_SRC):
        d, e = q // 2, q % 2
        to_one = lax.rem(core + e, 2)
        for m in range(RING):
            shard0 = dom_of(wrapped(y + d), wrapped(x - m), 0)
            shard1 = dom_of(wrapped(y - m), wrapped(x + d), 1)
            shard = jnp.where(to_one == 1, shard1, shard0)
            for s in range(CAP):
                stage[q, m * CAP + s] = ft[req[shard, s]]
        copy = pltpu.make_async_copy(stage.at[q], outs[q], sem.at[q])
        copy.start()
        copies.append(copy)
    for copy in copies:
        copy.wait()


def pack(me, requests, features):
    n_blk = features.shape[0] // ROWS
    return pl.pallas_call(
        pack_kernel,
        out_shape=[jax.ShapeDtypeStruct((RING * CAP, ROWS, ROWS), BF)] * N_SRC,
        in_specs=[SMEM, SMEM, VMEM],
        out_specs=[ANY] * N_SRC,
        scratch_shapes=[
            pltpu.VMEM((n_blk, ROWS, ROWS), BF),
            pltpu.VMEM((N_SRC, RING * CAP, ROWS, ROWS), BF),
            pltpu.SemaphoreType.DMA((N_SRC,)),
        ],
        cost_estimate=pl.CostEstimate(flops=10**9, bytes_accessed=10**7, transcendentals=0),
        name="pack",
    )(me, requests, features)


def tables_kernel(nbr, ws, wn, nbr_t, w_t):
    half = ROWS // 2

    def turn_nbr(i, _):
        turned = nbr[pl.ds(i * ROWS, ROWS), :].T
        nbr_t[pl.ds(i * half, half), :] = turned[:half] + turned[half:] * 65536
        return 0

    lax.fori_loop(0, nbr.shape[0] // ROWS, turn_nbr, 0, unroll=2)
    for j in range(D // ROWS):
        lanes = slice(j * ROWS, (j + 1) * ROWS)
        w_t[lanes, :ROWS] = ws[:, lanes].T
        w_t[lanes, ROWS:] = wn[:, lanes].T


def tables(local_nbr, w_self, w_neigh):
    return pl.pallas_call(
        tables_kernel,
        out_shape=(
            jax.ShapeDtypeStruct((local_nbr.shape[0] // 2, ROWS), I32),
            jax.ShapeDtypeStruct((D, 2 * ROWS), BF),
        ),
        in_specs=[VMEM] * 3,
        out_specs=(VMEM, VMEM),
        cost_estimate=pl.CostEstimate(flops=10**9, bytes_accessed=10**7, transcendentals=0),
        name="tables",
    )(local_nbr, w_self, w_neigh)


def plan_kernel(me, m0, m1, m2, m3, todo, size, own, slot):
    core, x, y = lax.rem(me[0], 2), lax.rem(me[0] // 2, RING), me[0] // (2 * RING)
    for q in range(N_SRC + 1):
        size[q] = 0
    for m, meta in enumerate((m0, m1, m2, m3)):

        def owner(o, p):
            co, xo, yo = lax.rem(o, 2), lax.rem(o // 2, RING), o // (2 * RING)
            q0 = wrapped(y - yo) * 2 + co
            q1 = wrapped(x - xo) * 2 + 1 - co
            q = jnp.where(core == 0, q0, q1)
            here = jnp.where(core == 0, xo == x, yo == y)
            first = jnp.where(here, q * 32 + m * CAP, N_SRC * 32)

            def one(s, p):
                slot[p] = first + s
                return p + 1

            return lax.fori_loop(0, meta[4, o], one, p)

        lax.fori_loop(0, 2 * RING * RING, owner, jnp.int32(0))

        def block(i, _):
            own[m * DST + i] = slot[i]

            def tile(t, _):
                v = slot[meta[i // 4, lax.rem(i, 4) * TILES + t]]
                q = v // 32
                n = size[q]
                todo[q * BUCKET + n] = lax.rem(v, 32) + 32 * (m * DST + i) + 4096 * t
                size[q] = n + 1
                return 0

            lax.fori_loop(0, meta[4, 32 + i], tile, 0)
            return 0

        lax.fori_loop(0, DST, block, 0)
    for q in range(N_SRC):
        for u in range(UNROLL - 1):
            todo[q * BUCKET + size[q] + u] = jnp.int32(32 * RING * DST)


def plan(me, metas):
    return pl.pallas_call(
        plan_kernel,
        out_shape=(
            jax.ShapeDtypeStruct(((N_SRC + 1) * BUCKET,), I32),
            jax.ShapeDtypeStruct((N_SRC + 1,), I32),
            jax.ShapeDtypeStruct((RING * DST,), I32),
        ),
        in_specs=[SMEM] * 5,
        out_specs=(SMEM, SMEM, SMEM),
        scratch_shapes=[pltpu.SMEM((FRONT,), I32)],
        cost_estimate=pl.CostEstimate(flops=2 * 10**9, bytes_accessed=10**6, transcendentals=0),
        name="plan",
    )(me, *metas)


def own_kernel(own, *refs):
    src, outs, (stage, sem, sem_out) = refs[:N_SRC], refs[N_SRC : N_SRC + RING], refs[N_SRC + RING :]

    def copy_of(q, n, v):
        return pltpu.make_async_copy(src[q].at[lax.rem(v, 32)], stage.at[n], sem)

    def start(n, _):
        v = own[n]
        for q in range(N_SRC):

            @pl.when(v // 32 == q)
            def _():
                copy_of(q, n, v).start()

        @pl.when(v // 32 == N_SRC)
        def _():
            stage[n] = jnp.zeros((ROWS, ROWS), BF)

        return 0

    lax.fori_loop(0, RING * DST, start, 0)

    def finish(n, _):
        @pl.when(own[n] // 32 < N_SRC)
        def _():
            copy_of(0, n, 0).wait()

        return 0

    lax.fori_loop(0, RING * DST, finish, 0)
    copies = [
        pltpu.make_async_copy(stage.at[pl.ds(m * DST, DST)], outs[m], sem_out.at[m]) for m in range(RING)
    ]
    for copy in copies:
        copy.start()
    for copy in copies:
        copy.wait()


def own_rows(own, sources):
    return pl.pallas_call(
        own_kernel,
        out_shape=[jax.ShapeDtypeStruct((DST, ROWS, ROWS), BF)] * RING,
        in_specs=[SMEM] + [ANY] * N_SRC,
        out_specs=[ANY] * RING,
        scratch_shapes=[
            pltpu.VMEM((RING * DST, ROWS, ROWS), BF),
            pltpu.SemaphoreType.DMA,
            pltpu.SemaphoreType.DMA((RING,)),
        ],
        cost_estimate=pl.CostEstimate(flops=10**9, bytes_accessed=10**7, transcendentals=0),
        name="own_rows",
    )(own, *sources)


def agg_kernel(todo, size, *refs):
    src, nbr, outs = refs[:N_SRC], refs[N_SRC : N_SRC + RING], refs[N_SRC + RING : N_SRC + 2 * RING]
    blocks, table, acc, sem, sem_t = refs[N_SRC + 2 * RING :]
    n_row = nbr[0].shape[0]
    loads = [pltpu.make_async_copy(nbr[m], table.at[pl.ds(m * n_row, n_row)], sem_t.at[m]) for m in range(RING)]
    fetch = [pltpu.make_async_copy(src[q], blocks.at[pl.ds(q * 32, 32)], sem.at[q]) for q in range(N_SRC)]
    for copy in loads + fetch:
        copy.start()

    def clear(n, _):
        acc[n] = jnp.zeros((ROWS, ROWS), F32)
        return 0

    lax.fori_loop(0, RING * DST + 1, clear, 0, unroll=5)
    for copy in loads:
        copy.wait()
    iota = lax.broadcasted_iota(I32, (ROWS, ROWS), 0).astype(F32).astype(BF)
    one, zero = jnp.ones((), BF), jnp.zeros((), BF)

    for q in range(N_SRC):
        fetch[q].wait()

        def some(h, _):
            parts = []
            for u in range(UNROLL):
                item = todo[q * BUCKET + h * UNROLL + u]
                blk = item & 31
                dst = (item >> 5) & 127
                t = item >> 12
                row0 = (blk >> 3) * n_row + (dst & 15) * (ROWS // 2) + (t & 15) * FAN_T
                shift = (t >> 4) * 16
                total = None
                for f in range(FAN_T):
                    row = (table[pl.ds(row0 + f, 1), :] >> shift) & 65535
                    hit = jnp.where(iota == row.astype(F32).astype(BF), one, zero)
                    total = hit if total is None else total + hit
                parts.append((dst, jnp.dot(blocks[q * 32 + blk], total, preferred_element_type=F32)))
            for dst, part in parts:
                acc[dst] += part
            return 0

        lax.fori_loop(0, (size[q] + UNROLL - 1) // UNROLL, some, 0)
    for m in range(RING):

        def leave(n, _):
            outs[m][n] = acc[m * DST + n].astype(BF)
            return 0

        lax.fori_loop(0, DST, leave, 0, unroll=4)


def aggregate(todo, size, sources, nbrs):
    n_row = nbrs[0].shape[0]
    return pl.pallas_call(
        agg_kernel,
        out_shape=[jax.ShapeDtypeStruct((DST, ROWS, ROWS), BF)] * RING,
        in_specs=[SMEM, SMEM] + [ANY] * (N_SRC + RING),
        out_specs=[VMEM] * RING,
        scratch_shapes=[
            pltpu.VMEM((N_SRC * 32, ROWS, ROWS), BF),
            pltpu.VMEM((RING * n_row, ROWS), I32),
            pltpu.VMEM((RING * DST + 1, ROWS, ROWS), F32),
            pltpu.SemaphoreType.DMA((N_SRC,)),
            pltpu.SemaphoreType.DMA((RING,)),
        ],
        cost_estimate=pl.CostEstimate(flops=10**10, bytes_accessed=2 * 10**7, transcendentals=0),
        name="agg",
    )(todo, size, *sources, *nbrs)


def join_own_kernel(a, b, c, d, out):
    for n in range(DST):
        total = a[n].astype(F32) + b[n].astype(F32) + c[n].astype(F32) + d[n].astype(F32)
        out[n] = total.astype(BF)


def join_agg_kernel(tile_count, a, b, c, d, out):
    for n in range(DST):
        total = a[n].astype(F32) + b[n].astype(F32) + c[n].astype(F32) + d[n].astype(F32)
        out[n] = (total / (tile_count[n] * FAN_T).astype(F32)).astype(BF)


def join(kernel, name, scalars, parts):
    return pl.pallas_call(
        kernel,
        out_shape=jax.ShapeDtypeStruct((DST, ROWS, ROWS), BF),
        in_specs=[SMEM] * len(scalars) + [VMEM] * RING,
        out_specs=VMEM,
        cost_estimate=pl.CostEstimate(flops=10**9, bytes_accessed=5 * 10**6, transcendentals=0),
        name=name,
    )(*scalars, *parts)


def project_kernel(me, xs, xa, *refs):
    *w_t, out, hid = refs
    n_col = xs.shape[0]
    for b in range(xs.shape[1]):
        for n0 in range(0, D, 256):
            total = None
            for k in range(n_col):
                group = lax.rem(me[0] + n_col - k, n_col)
                both = jnp.concatenate([xs[group, b], xa[group, b]], axis=0)
                part = jnp.dot(w_t[k][n0 : n0 + 256, :], both, preferred_element_type=F32)
                total = part if total is None else total + part
            hid[n0 : n0 + 256, :] = jnp.maximum(total, 0.0)
        h = hid[...]
        scale = jnp.sqrt(0.25 + jnp.sum(h * h, axis=0, keepdims=True) / D)
        for j in range(n_col):
            piece = hid[j * ROWS : (j + 1) * ROWS, :] / scale
            out[j, b * ROWS : (b + 1) * ROWS, :] = piece.T.astype(BF)


def project(me, xs, xa, w_t):
    n_col, n_blk = xs.shape[:2]
    return pl.pallas_call(
        project_kernel,
        out_shape=jax.ShapeDtypeStruct((n_col, n_blk * ROWS, ROWS), BF),
        in_specs=[SMEM] + [VMEM] * (2 + n_col),
        out_specs=VMEM,
        scratch_shapes=[pltpu.VMEM((D, ROWS), F32)],
        cost_estimate=pl.CostEstimate(flops=10**9, bytes_accessed=5 * 10**6, transcendentals=0),
        name="project",
    )(me, xs, xa, *w_t)


def on_device(features, requests, counts, tile_block, local_nbr, tile_count, w_self, w_neigh):
    n_col = lax.axis_size("col")
    me = lax.axis_index("dom").reshape(1).astype(I32)
    column = lax.axis_index("col").reshape(1).astype(I32)
    packed = pack(me, requests[0], features)
    sources = [packed[0]]
    for q in range(1, N_SRC):
        sources.append(lax.ppermute(packed[q], "dom", meet_pairs(q // 2, q % 2)))

    counted = jnp.concatenate([counts[:, 0], tile_count, jnp.zeros((ROWS - 48,), I32)])
    meta = jnp.concatenate([tile_block.reshape(RING, ROWS), counted[None]])
    nbr_t, w_t = tables(local_nbr, w_self, w_neigh)
    metas, nbrs = [meta], [nbr_t]
    for m in range(1, RING):
        metas.append(lax.ppermute(meta, "dom", ring_pairs(m)))
        nbrs.append(lax.ppermute(nbr_t, "dom", ring_pairs(m)))
    w_all = [w_t]
    for k in range(1, n_col):
        w_all.append(lax.ppermute(w_t, "col", [(i, (i + k) % n_col) for i in range(n_col)]))
    todo, size, own = plan(me, metas)

    own_parts = own_rows(own, sources)
    own_here = [own_parts[0]]
    for m in range(1, RING):
        own_here.append(lax.ppermute(own_parts[m], "dom", ring_pairs(RING - m)))
    agg_parts = aggregate(todo, size, sources, nbrs)
    agg_here = [agg_parts[0]]
    for m in range(1, RING):
        agg_here.append(lax.ppermute(agg_parts[m], "dom", ring_pairs(RING - m)))

    def to_rows(x):
        return lax.all_to_all(x.reshape(n_col, DST // n_col, ROWS, ROWS), "col", 0, 0, tiled=True)

    xs = to_rows(join(join_own_kernel, "join_own", (), own_here))
    xa = to_rows(join(join_agg_kernel, "join_agg", (tile_count,), agg_here))
    y = project(column, xs, xa, w_all)
    return lax.all_to_all(y, "col", 0, 0, tiled=True).reshape(-1, ROWS)


def solution(mesh):
    return jax.shard_map(
        on_device,
        mesh=mesh,
        in_specs=(
            P("dom", "col"),
            P("dom", None, None),
            P(None, "dom"),
            P("dom", None),
            P("dom", None),
            P("dom"),
            P("col", None),
            P("col", None),
        ),
        out_specs=P("dom", "col"),
        check_vma=False,
    )
```

```python
import jax
import jax.numpy as jnp
from jax import lax
from jax.experimental import pallas as pl
from jax.experimental.pallas import tpu as pltpu
from jax.sharding import PartitionSpec as P


D = 1024
ROWS = 128
CAP = 8
TILES = 32
FAN_T = 4
FRONT = 128
RING = 4
N_SRC = 2 * RING
DST = 16
N_ITEMS = DST * TILES
SECTION = N_ITEMS + ROWS
UNROLL = 4
BF = jnp.bfloat16
F32 = jnp.float32
I32 = jnp.int32

VMEM = pl.BlockSpec(memory_space=pltpu.VMEM)
SMEM = pl.BlockSpec(memory_space=pltpu.SMEM)
ANY = pl.BlockSpec(memory_space=pl.ANY)


def dom_of(y, x, core):
    return (y * RING + x) * 2 + core


def meet_pairs(d, e):
    pairs = []
    for y in range(RING):
        for x in range(RING):
            for core in range(2):
                if core ^ e == 0:
                    pairs.append((dom_of(y, x, core), dom_of((y + d) % RING, x, 0)))
                else:
                    pairs.append((dom_of(y, x, core), dom_of(y, (x + d) % RING, 1)))
    return pairs


def ring_pairs(m):
    pairs = []
    for y in range(RING):
        for x in range(RING):
            pairs.append((dom_of(y, x, 0), dom_of(y, (x + m) % RING, 0)))
            pairs.append((dom_of(y, x, 1), dom_of((y + m) % RING, x, 1)))
    return pairs


def wrapped(v):
    return lax.rem(v + 2 * RING, RING)


def pack_kernel(me, req, feat, *refs):
    outs, (ft, stage, sem) = refs[:N_SRC], refs[N_SRC:]
    core, x, y = lax.rem(me[0], 2), lax.rem(me[0] // 2, RING), me[0] // (2 * RING)

    def turn(b, _):
        for u in range(8):
            ft[b * 8 + u] = feat[pl.ds((b * 8 + u) * ROWS, ROWS), :].T
        return 0

    lax.fori_loop(0, feat.shape[0] // ROWS // 8, turn, 0)
    copies = []
    for q in range(N_SRC):
        d, e = q // 2, q % 2
        to_one = lax.rem(core + e, 2)
        for m in range(RING):
            shard0 = dom_of(wrapped(y + d), wrapped(x - m), 0)
            shard1 = dom_of(wrapped(y - m), wrapped(x + d), 1)
            shard = jnp.where(to_one == 1, shard1, shard0)
            for s in range(CAP):
                stage[q, m * CAP + s] = ft[req[shard, s]]
        copy = pltpu.make_async_copy(stage.at[q], outs[q], sem.at[q])
        copy.start()
        copies.append(copy)
    for copy in copies:
        copy.wait()


def pack(me, requests, features):
    n_blk = features.shape[0] // ROWS
    return pl.pallas_call(
        pack_kernel,
        out_shape=[jax.ShapeDtypeStruct((RING * CAP, ROWS, ROWS), BF)] * N_SRC,
        in_specs=[SMEM, SMEM, VMEM],
        out_specs=[ANY] * N_SRC,
        scratch_shapes=[
            pltpu.VMEM((n_blk, ROWS, ROWS), BF),
            pltpu.VMEM((N_SRC, RING * CAP, ROWS, ROWS), BF),
            pltpu.SemaphoreType.DMA((N_SRC,)),
        ],
        cost_estimate=pl.CostEstimate(flops=10**9, bytes_accessed=10**7, transcendentals=0),
        name="pack",
    )(me, requests, features)


def tables_kernel(me, nbr, ws, wn, nbr_t, w_t):
    half = ROWS // 2

    def turn_nbr(i, _):
        turned = nbr[pl.ds(i * ROWS, ROWS), :].T
        nbr_t[pl.ds(i * half, half), :] = turned[:half] + turned[half:] * 65536
        return 0

    lax.fori_loop(0, nbr.shape[0] // ROWS, turn_nbr, 0, unroll=2)
    for core, w in enumerate((ws, wn)):

        @pl.when(lax.rem(me[0], 2) == core)
        def _():
            for j in range(D // ROWS):
                w_t[j * ROWS : (j + 1) * ROWS, :] = w[:, j * ROWS : (j + 1) * ROWS].T


def tables(me, local_nbr, w_self, w_neigh):
    return pl.pallas_call(
        tables_kernel,
        out_shape=(
            jax.ShapeDtypeStruct((local_nbr.shape[0] // 2, ROWS), I32),
            jax.ShapeDtypeStruct((D, ROWS), BF),
        ),
        in_specs=[SMEM] + [VMEM] * 3,
        out_specs=(VMEM, VMEM),
        cost_estimate=pl.CostEstimate(flops=10**9, bytes_accessed=10**7, transcendentals=0),
        name="tables",
    )(me, local_nbr, w_self, w_neigh)


def plan_kernel(me, cnt, tile_block, tile_count, todo, slot, size):
    core, x, y = me[0] & 1, (me[0] >> 1) & (RING - 1), me[0] >> 3
    for m in range(RING + 1):
        size[m] = m * SECTION

    def owner(o, p):
        co, xo, yo = o & 1, (o >> 1) & (RING - 1), o >> 3
        q0 = ((y - yo) & (RING - 1)) * 2 + co
        q1 = ((x - xo) & (RING - 1)) * 2 + 1 - co
        q = jnp.where(core == 0, q0, q1)
        m = jnp.where(core == 0, xo - x, yo - y) & (RING - 1)
        first = q * 32 + m * CAP

        def one(s, p):
            slot[p] = first + s
            return p + 1

        return lax.fori_loop(0, cnt[o], one, p)

    lax.fori_loop(0, 2 * RING * RING, owner, jnp.int32(0))

    def block(i, _):
        v = slot[i]
        for m in range(RING):
            todo[m * SECTION + N_ITEMS + 1 + i] = jnp.where((v >> 3) & (RING - 1) == m, v, -1)
        used = tile_count[i]

        def tile(h, _):
            vs = [slot[tile_block[i, h * UNROLL + u]] for u in range(UNROLL)]
            for u, v in enumerate(vs):
                t = h * UNROLL + u
                m = jnp.where(t < used, (v >> 3) & (RING - 1), RING)
                n = size[m]
                todo[n] = v + 256 * i + 4096 * t
                size[m] = n + 1
            return 0

        lax.fori_loop(0, (used + UNROLL - 1) // UNROLL, tile, 0)
        return 0

    lax.fori_loop(0, DST, block, 0)
    for m in range(RING):
        todo[m * SECTION + N_ITEMS] = size[m] - m * SECTION


def plan(me, counts, tile_block, tile_count):
    return pl.pallas_call(
        plan_kernel,
        out_shape=jax.ShapeDtypeStruct(((RING + 1) * SECTION,), I32),
        in_specs=[SMEM] * 4,
        out_specs=SMEM,
        scratch_shapes=[pltpu.SMEM((FRONT,), I32), pltpu.SMEM((RING + 1,), I32)],
        cost_estimate=pl.CostEstimate(flops=2 * 10**9, bytes_accessed=10**6, transcendentals=0),
        name="plan",
    )(me, counts, tile_block, tile_count)


def own_kernel(*refs):
    lists, src, outs = refs[:RING], refs[RING : RING + N_SRC], refs[RING + N_SRC : 2 * RING + N_SRC]
    stage, sem, sem_out = refs[2 * RING + N_SRC :]

    def copy_of(q, n, v):
        return pltpu.make_async_copy(src[q].at[v & 31], stage.at[n], sem)

    for m in range(RING):

        def start(i, _):
            v = lists[m][m * SECTION + N_ITEMS + 1 + i]
            for q in range(N_SRC):

                @pl.when(v >> 5 == q)
                def _():
                    copy_of(q, m * DST + i, v).start()

            @pl.when(v < 0)
            def _():
                stage[m * DST + i] = jnp.zeros((ROWS, ROWS), BF)

            return 0

        lax.fori_loop(0, DST, start, 0)
    for m in range(RING):

        def finish(i, _):
            @pl.when(lists[m][m * SECTION + N_ITEMS + 1 + i] >= 0)
            def _():
                copy_of(0, 0, 0).wait()

            return 0

        lax.fori_loop(0, DST, finish, 0)
    copies = [
        pltpu.make_async_copy(stage.at[pl.ds(m * DST, DST)], outs[m], sem_out.at[m]) for m in range(RING)
    ]
    for copy in copies:
        copy.start()
    for copy in copies:
        copy.wait()


def own_rows(lists, sources):
    return pl.pallas_call(
        own_kernel,
        out_shape=[jax.ShapeDtypeStruct((DST, ROWS, ROWS), BF)] * RING,
        in_specs=[SMEM] * RING + [ANY] * N_SRC,
        out_specs=[ANY] * RING,
        scratch_shapes=[
            pltpu.VMEM((RING * DST, ROWS, ROWS), BF),
            pltpu.SemaphoreType.DMA,
            pltpu.SemaphoreType.DMA((RING,)),
        ],
        cost_estimate=pl.CostEstimate(flops=10**9, bytes_accessed=10**7, transcendentals=0),
        name="own_rows",
    )(*lists, *sources)


def agg_kernel(*refs):
    lists, src, nbr = refs[:RING], refs[RING : RING + N_SRC], refs[RING + N_SRC : 2 * RING + N_SRC]
    outs, (blocks, acc, sem) = refs[2 * RING + N_SRC : 3 * RING + N_SRC], refs[3 * RING + N_SRC :]
    fetch = [pltpu.make_async_copy(src[q], blocks.at[pl.ds(q * 32, 32)], sem.at[q]) for q in range(N_SRC)]
    for copy in fetch:
        copy.start()

    def clear(n, _):
        acc[n] = jnp.zeros((ROWS, ROWS), F32)
        return 0

    lax.fori_loop(0, RING * DST + 1, clear, 0, unroll=5)
    iota = lax.broadcasted_iota(I32, (ROWS, ROWS), 0).astype(F32).astype(BF)
    one, zero = jnp.ones((), BF), jnp.zeros((), BF)
    for copy in fetch:
        copy.wait()

    for m in (1, 2, 3, 0):
        todo = lists[m]
        n_item = todo[m * SECTION + N_ITEMS]

        def some(h, _):
            parts = []
            for u in range(UNROLL):
                n = h * UNROLL + u
                item = jnp.where(n < n_item, todo[m * SECTION + n], 0)
                blk = item & 255
                i = (item >> 8) & 15
                t = item >> 12
                dst = jnp.where(n < n_item, m * DST + i, RING * DST)
                row0 = i * (ROWS // 2) + (t & 15) * FAN_T
                shift = (t >> 4) * 16
                total = None
                for f in range(FAN_T):
                    row = (nbr[m][pl.ds(row0 + f, 1), :] >> shift) & 65535
                    hit = jnp.where(iota == row.astype(F32).astype(BF), one, zero)
                    total = hit if total is None else total + hit
                parts.append((dst, jnp.dot(blocks[blk], total, preferred_element_type=F32)))
            for dst, part in parts:
                acc[dst] += part
            return 0

        lax.fori_loop(0, (n_item + UNROLL - 1) // UNROLL, some, 0)
    for m in range(RING):

        def leave(n, _):
            outs[m][n] = acc[m * DST + n].astype(BF)
            return 0

        lax.fori_loop(0, DST, leave, 0, unroll=4)


def aggregate(lists, sources, nbrs):
    return pl.pallas_call(
        agg_kernel,
        out_shape=[jax.ShapeDtypeStruct((DST, ROWS, ROWS), BF)] * RING,
        in_specs=[SMEM] * RING + [ANY] * N_SRC + [VMEM] * RING,
        out_specs=[VMEM] * RING,
        scratch_shapes=[
            pltpu.VMEM((N_SRC * 32, ROWS, ROWS), BF),
            pltpu.VMEM((RING * DST + 1, ROWS, ROWS), F32),
            pltpu.SemaphoreType.DMA((N_SRC,)),
        ],
        cost_estimate=pl.CostEstimate(flops=10**10, bytes_accessed=2 * 10**7, transcendentals=0),
        name="agg",
    )(*lists, *sources, *nbrs)


def join_own_kernel(a, b, c, d, out):
    for n in range(DST):
        total = a[n].astype(F32) + b[n].astype(F32) + c[n].astype(F32) + d[n].astype(F32)
        out[n] = total.astype(BF)


def join_agg_kernel(tile_count, a, b, c, d, out):
    for n in range(DST):
        total = a[n].astype(F32) + b[n].astype(F32) + c[n].astype(F32) + d[n].astype(F32)
        out[n] = (total / (tile_count[n] * FAN_T).astype(F32)).astype(BF)


def join(kernel, scalars, parts):
    return pl.pallas_call(
        kernel,
        out_shape=jax.ShapeDtypeStruct((DST, ROWS, ROWS), BF),
        in_specs=[SMEM] * len(scalars) + [VMEM] * RING,
        out_specs=VMEM,
        cost_estimate=pl.CostEstimate(flops=10**9, bytes_accessed=5 * 10**6, transcendentals=0),
    )(*scalars, *parts)


def gather_kernel(*refs):
    *parts, out = refs
    for k, part in enumerate(parts):
        out[k] = part[...]


def gather_weights(parts):
    return pl.pallas_call(
        gather_kernel,
        out_shape=jax.ShapeDtypeStruct((len(parts), *parts[0].shape), BF),
        in_specs=[VMEM] * len(parts),
        out_specs=VMEM,
        cost_estimate=pl.CostEstimate(flops=10**9, bytes_accessed=5 * 10**6, transcendentals=0),
        name="gather_weights",
    )(*parts)


def project_kernel(me, column, xs, xa, w_mine, w_other, out, hid):
    n_col = xs.shape[0]
    self_first = me[0] & 1 == 0
    for b in range(xs.shape[1]):
        for n0 in range(0, D, 256):
            total = None
            for k in range(n_col):
                group = (column[0] + n_col - k) & (n_col - 1)
                s, a = xs[group, b], xa[group, b]
                x = jnp.concatenate([jnp.where(self_first, s, a), jnp.where(self_first, a, s)], axis=0)
                w = jnp.concatenate([w_mine[k, n0 : n0 + 256, :], w_other[k, n0 : n0 + 256, :]], axis=1)
                part = jnp.dot(w, x, preferred_element_type=F32)
                total = part if total is None else total + part
            hid[n0 : n0 + 256, :] = jnp.maximum(total, 0.0)
        h = hid[...]
        scale = jnp.sqrt(0.25 + jnp.sum(h * h, axis=0, keepdims=True) / D)
        for j in range(n_col):
            piece = hid[j * ROWS : (j + 1) * ROWS, :] / scale
            out[j, b * ROWS : (b + 1) * ROWS, :] = piece.T.astype(BF)


def project(me, column, xs, xa, w_mine, w_other):
    n_col, n_blk = xs.shape[:2]
    return pl.pallas_call(
        project_kernel,
        out_shape=jax.ShapeDtypeStruct((n_col, n_blk * ROWS, ROWS), BF),
        in_specs=[SMEM] * 2 + [VMEM] * 4,
        out_specs=VMEM,
        scratch_shapes=[pltpu.VMEM((D, ROWS), F32)],
        cost_estimate=pl.CostEstimate(flops=10**9, bytes_accessed=5 * 10**6, transcendentals=0),
        name="project",
    )(me, column, xs, xa, w_mine, w_other)


def body(features, requests, counts, tile_block, local_nbr, tile_count, w_self, w_neigh):
    n_col = lax.axis_size("col")
    me = lax.axis_index("dom").reshape(1).astype(I32)
    column = lax.axis_index("col").reshape(1).astype(I32)
    packed = pack(me, requests[0], features)
    sources = [packed[0]]
    for q in range(1, N_SRC):
        sources.append(lax.ppermute(packed[q], "dom", meet_pairs(q // 2, q % 2)))

    todo = plan(me, counts[:, 0], tile_block, tile_count)
    nbr_t, w_t = tables(me, local_nbr, w_self, w_neigh)
    lists, nbrs = [todo], [nbr_t]
    for m in range(1, RING):
        lists.append(lax.ppermute(todo, "dom", ring_pairs(m)))
        nbrs.append(lax.ppermute(nbr_t, "dom", ring_pairs(m)))
    w_all = [w_t]
    for k in range(1, n_col):
        w_all.append(lax.ppermute(w_t, "col", [(i, (i + k) % n_col) for i in range(n_col)]))
    w_mine = gather_weights(w_all)
    w_other = lax.ppermute(w_mine, "dom", [(i, i ^ 1) for i in range(lax.axis_size("dom"))])

    own_parts = own_rows(lists, sources)
    own_here = [own_parts[0]]
    for m in range(1, RING):
        own_here.append(lax.ppermute(own_parts[m], "dom", ring_pairs(RING - m)))
    agg_parts = aggregate(lists, sources, nbrs)
    agg_here = [agg_parts[0]]
    for m in range(1, RING):
        agg_here.append(lax.ppermute(agg_parts[m], "dom", ring_pairs(RING - m)))

    def to_rows(x):
        return lax.all_to_all(x.reshape(n_col, DST // n_col, ROWS, ROWS), "col", 0, 0, tiled=True)

    xs = to_rows(join(join_own_kernel, (), own_here))
    xa = to_rows(join(join_agg_kernel, (tile_count,), agg_here))
    y = project(me, column, xs, xa, w_mine, w_other)
    return lax.all_to_all(y, "col", 0, 0, tiled=True).reshape(-1, ROWS)


def solution(mesh):
    return jax.shard_map(
        body,
        mesh=mesh,
        in_specs=(
            P("dom", "col"),
            P("dom", None, None),
            P(None, "dom"),
            P("dom", None),
            P("dom", None),
            P("dom"),
            P("col", None),
            P("col", None),
        ),
        out_specs=P("dom", "col"),
        check_vma=False,
    )
```

```python
import functools

import jax
import jax.numpy as jnp
from jax import lax
from jax.experimental import pallas as pl
from jax.experimental.pallas import tpu as pltpu
from jax.sharding import PartitionSpec as P


D = 1024
ROWS = 128
CAP = 8
TILES = 32
FAN_T = 4
FRONT = 128
RING = 4
N_SRC = 2 * RING
DST = 16
N_ITEMS = DST * TILES
SECTION = N_ITEMS + ROWS
UNROLL = 4
JOIN = 4
BF = jnp.bfloat16
F32 = jnp.float32
I32 = jnp.int32

VMEM = pl.BlockSpec(memory_space=pltpu.VMEM)
SMEM = pl.BlockSpec(memory_space=pltpu.SMEM)
ANY = pl.BlockSpec(memory_space=pl.ANY)


def dom_of(y, x, core):
    return (y * RING + x) * 2 + core


def meet_pairs(d, e):
    pairs = []
    for y in range(RING):
        for x in range(RING):
            for core in range(2):
                if core ^ e == 0:
                    pairs.append((dom_of(y, x, core), dom_of((y + d) % RING, x, 0)))
                else:
                    pairs.append((dom_of(y, x, core), dom_of(y, (x + d) % RING, 1)))
    return pairs


def ring_pairs(m):
    pairs = []
    for y in range(RING):
        for x in range(RING):
            pairs.append((dom_of(y, x, 0), dom_of(y, (x + m) % RING, 0)))
            pairs.append((dom_of(y, x, 1), dom_of((y + m) % RING, x, 1)))
    return pairs


def wrapped(v):
    return lax.rem(v + 2 * RING, RING)


def pack_kernel(me, req, feat, *refs):
    outs, (ft, stage, sem) = refs[:N_SRC], refs[N_SRC:]
    core, x, y = lax.rem(me[0], 2), lax.rem(me[0] // 2, RING), me[0] // (2 * RING)

    def turn(b, _):
        for u in range(8):
            ft[b * 8 + u] = feat[pl.ds((b * 8 + u) * ROWS, ROWS), :].T
        return 0

    lax.fori_loop(0, feat.shape[0] // ROWS // 8, turn, 0)
    copies = []
    for q in range(N_SRC):
        d, e = q // 2, q % 2
        to_one = lax.rem(core + e, 2)
        for m in range(RING):
            shard0 = dom_of(wrapped(y + d), wrapped(x - m), 0)
            shard1 = dom_of(wrapped(y - m), wrapped(x + d), 1)
            shard = jnp.where(to_one == 1, shard1, shard0)
            for s in range(CAP):
                stage[q, m * CAP + s] = ft[req[s, shard]]
        copy = pltpu.make_async_copy(stage.at[q], outs[q], sem.at[q])
        copy.start()
        copies.append(copy)
    for copy in copies:
        copy.wait()


def pack(me, requests, features):
    n_blk = features.shape[0] // ROWS
    return pl.pallas_call(
        pack_kernel,
        out_shape=[jax.ShapeDtypeStruct((RING * CAP, ROWS, ROWS), BF)] * N_SRC,
        in_specs=[SMEM, SMEM, VMEM],
        out_specs=[ANY] * N_SRC,
        scratch_shapes=[
            pltpu.VMEM((n_blk, ROWS, ROWS), BF),
            pltpu.VMEM((N_SRC, RING * CAP, ROWS, ROWS), BF),
            pltpu.SemaphoreType.DMA((N_SRC,)),
        ],
        cost_estimate=pl.CostEstimate(flops=10**9, bytes_accessed=10**7, transcendentals=0),
        name="pack",
    )(me, requests, features)


def tables_kernel(me, nbr, ws, wn, nbr_t, w_t):
    half = ROWS // 2

    def turn_nbr(i, _):
        turned = nbr[pl.ds(i * ROWS, ROWS), :].T
        nbr_t[pl.ds(i * half, half), :] = turned[:half] + turned[half:] * 65536
        return 0

    lax.fori_loop(0, nbr.shape[0] // ROWS, turn_nbr, 0, unroll=2)
    for core, w in enumerate((ws, wn)):

        @pl.when(lax.rem(me[0], 2) == core)
        def _():
            for j in range(D // ROWS):
                w_t[j * ROWS : (j + 1) * ROWS, :] = w[:, j * ROWS : (j + 1) * ROWS].T


def tables(me, local_nbr, w_self, w_neigh):
    return pl.pallas_call(
        tables_kernel,
        out_shape=(
            jax.ShapeDtypeStruct((local_nbr.shape[0] // 2, ROWS), I32),
            jax.ShapeDtypeStruct((D, ROWS), BF),
        ),
        in_specs=[SMEM] + [VMEM] * 3,
        out_specs=(VMEM, VMEM),
        cost_estimate=pl.CostEstimate(flops=10**9, bytes_accessed=10**7, transcendentals=0),
        name="tables",
    )(me, local_nbr, w_self, w_neigh)


def plan_kernel(me, cnt, tile_block, tile_count, todo, slot, size):
    core, x, y = me[0] & 1, (me[0] >> 1) & (RING - 1), me[0] >> 3
    for m in range(RING + 1):
        size[m] = m * SECTION

    def owner(o, p):
        co, xo, yo = o & 1, (o >> 1) & (RING - 1), o >> 3
        q0 = ((y - yo) & (RING - 1)) * 2 + co
        q1 = ((x - xo) & (RING - 1)) * 2 + 1 - co
        q = jnp.where(core == 0, q0, q1)
        m = jnp.where(core == 0, xo - x, yo - y) & (RING - 1)
        first = q * 32 + m * CAP

        def one(s, p):
            slot[p] = first + s
            return p + 1

        return lax.fori_loop(0, cnt[o], one, p)

    lax.fori_loop(0, 2 * RING * RING, owner, jnp.int32(0))

    def block(i, _):
        v = slot[i]
        for m in range(RING):
            todo[m * SECTION + N_ITEMS + 1 + i] = jnp.where((v >> 3) & (RING - 1) == m, v, -1)
        used = tile_count[i]

        def tile(h, _):
            vs = [slot[tile_block[i, h * UNROLL + u]] for u in range(UNROLL)]
            for u, v in enumerate(vs):
                t = h * UNROLL + u
                m = jnp.where(t < used, (v >> 3) & (RING - 1), RING)
                n = size[m]
                todo[n] = v + 256 * i + 4096 * t
                size[m] = n + 1
            return 0

        lax.fori_loop(0, (used + UNROLL - 1) // UNROLL, tile, 0)
        return 0

    lax.fori_loop(0, DST, block, 0)
    for m in range(RING):
        todo[m * SECTION + N_ITEMS] = size[m] - m * SECTION


def plan(me, counts, tile_block, tile_count):
    return pl.pallas_call(
        plan_kernel,
        out_shape=jax.ShapeDtypeStruct(((RING + 1) * SECTION,), I32),
        in_specs=[SMEM] * 4,
        out_specs=SMEM,
        scratch_shapes=[pltpu.SMEM((FRONT,), I32), pltpu.SMEM((RING + 1,), I32)],
        cost_estimate=pl.CostEstimate(flops=2 * 10**9, bytes_accessed=10**6, transcendentals=0),
        name="plan",
    )(me, counts, tile_block, tile_count)


def own_kernel(*refs):
    lists, src, outs = refs[:RING], refs[RING : RING + N_SRC], refs[RING + N_SRC : 2 * RING + N_SRC]
    stage, sem, sem_out = refs[2 * RING + N_SRC :]

    def copy_of(q, n, v):
        return pltpu.make_async_copy(src[q].at[v & 31], stage.at[n], sem)

    for m in range(RING):

        def start(i, _):
            v = lists[m][m * SECTION + N_ITEMS + 1 + i]

            @pl.when(v >= 0)
            def _():
                for q in range(N_SRC):

                    @pl.when(v >> 5 == q)
                    def _():
                        copy_of(q, m * DST + i, v).start()

            @pl.when(v < 0)
            def _():
                stage[m * DST + i] = jnp.zeros((ROWS, ROWS), BF)

            return 0

        lax.fori_loop(0, DST, start, 0)
    for m in range(RING):

        def finish(i, _):
            @pl.when(lists[m][m * SECTION + N_ITEMS + 1 + i] >= 0)
            def _():
                copy_of(0, 0, 0).wait()

            return 0

        lax.fori_loop(0, DST, finish, 0)
    copies = [
        pltpu.make_async_copy(stage.at[pl.ds(m * DST, DST)], outs[m], sem_out.at[m]) for m in range(RING)
    ]
    for copy in copies:
        copy.start()
    for copy in copies:
        copy.wait()


def own_rows(lists, sources):
    return pl.pallas_call(
        own_kernel,
        out_shape=[jax.ShapeDtypeStruct((DST, ROWS, ROWS), BF)] * RING,
        in_specs=[SMEM] * RING + [ANY] * N_SRC,
        out_specs=[ANY] * RING,
        scratch_shapes=[
            pltpu.VMEM((RING * DST, ROWS, ROWS), BF),
            pltpu.SemaphoreType.DMA,
            pltpu.SemaphoreType.DMA((RING,)),
        ],
        cost_estimate=pl.CostEstimate(flops=10**9, bytes_accessed=10**7, transcendentals=0),
        name="own_rows",
    )(*lists, *sources)


def agg_kernel(m, todo, *refs):
    src, nbr, out, (blocks, acc, sem) = refs[:N_SRC], refs[N_SRC], refs[N_SRC + 1], refs[N_SRC + 2 :]
    fetch = [
        pltpu.make_async_copy(src[q].at[pl.ds(m * CAP, CAP)], blocks.at[pl.ds(q * CAP, CAP)], sem.at[q])
        for q in range(N_SRC)
    ]
    for copy in fetch:
        copy.start()

    def clear(n, _):
        acc[n] = jnp.zeros((ROWS, ROWS), F32)
        return 0

    lax.fori_loop(0, DST + 1, clear, 0)
    iota = lax.broadcasted_iota(I32, (ROWS, ROWS), 0).astype(F32).astype(BF)
    one, zero = jnp.ones((), BF), jnp.zeros((), BF)
    n_item = todo[m * SECTION + N_ITEMS]
    for copy in fetch:
        copy.wait()

    def some(h, _):
        parts = []
        for u in range(UNROLL):
            n = h * UNROLL + u
            item = jnp.where(n < n_item, todo[m * SECTION + n], 0)
            blk = ((item >> 5) & 7) * CAP + (item & 7)
            i = (item >> 8) & 15
            t = item >> 12
            row0 = i * (ROWS // 2) + (t & 15) * FAN_T
            shift = (t >> 4) * 16
            total = None
            for f in range(FAN_T):
                row = (nbr[pl.ds(row0 + f, 1), :] >> shift) & 65535
                hit = jnp.where(iota == row.astype(F32).astype(BF), one, zero)
                total = hit if total is None else total + hit
            dst = jnp.where(n < n_item, i, DST)
            parts.append((dst, jnp.dot(blocks[blk], total, preferred_element_type=F32)))
        for dst, part in parts:
            acc[dst] += part
        return 0

    lax.fori_loop(0, (n_item + UNROLL - 1) // UNROLL, some, 0)

    def leave(n, _):
        out[n] = acc[n].astype(BF)
        return 0

    lax.fori_loop(0, DST, leave, 0, unroll=4)


def aggregate(m, todo, sources, nbr_t):
    return pl.pallas_call(
        functools.partial(agg_kernel, m),
        out_shape=jax.ShapeDtypeStruct((DST, ROWS, ROWS), BF),
        in_specs=[SMEM] + [ANY] * N_SRC + [VMEM],
        out_specs=VMEM,
        scratch_shapes=[
            pltpu.VMEM((N_SRC * CAP, ROWS, ROWS), BF),
            pltpu.VMEM((DST + 1, ROWS, ROWS), F32),
            pltpu.SemaphoreType.DMA((N_SRC,)),
        ],
        cost_estimate=pl.CostEstimate(flops=4 * 10**9, bytes_accessed=5 * 10**6, transcendentals=0),
    )(todo, *sources, nbr_t)


def join_own_kernel(a, b, c, d, out):
    total = a[...].astype(F32) + b[...].astype(F32) + c[...].astype(F32) + d[...].astype(F32)
    out[...] = total.astype(BF)


def join_agg_kernel(tile_count, a, b, c, d, out):
    step = pl.program_id(0)
    for n in range(JOIN):
        total = a[n].astype(F32) + b[n].astype(F32) + c[n].astype(F32) + d[n].astype(F32)
        out[n] = (total / (tile_count[step * JOIN + n] * FAN_T).astype(F32)).astype(BF)


def join(kernel, scalars, parts):
    some = pl.BlockSpec((JOIN, ROWS, ROWS), lambda g: (g, 0, 0))
    return pl.pallas_call(
        kernel,
        grid=(DST // JOIN,),
        out_shape=jax.ShapeDtypeStruct((DST, ROWS, ROWS), BF),
        in_specs=[SMEM] * len(scalars) + [some] * RING,
        out_specs=some,
        cost_estimate=pl.CostEstimate(flops=10**9, bytes_accessed=5 * 10**6, transcendentals=0),
    )(*scalars, *parts)


def gather_kernel(*refs):
    *parts, out = refs
    for k, part in enumerate(parts):
        out[k] = part[...]


def gather_weights(parts):
    return pl.pallas_call(
        gather_kernel,
        out_shape=jax.ShapeDtypeStruct((len(parts), *parts[0].shape), BF),
        in_specs=[VMEM] * len(parts),
        out_specs=VMEM,
        cost_estimate=pl.CostEstimate(flops=10**9, bytes_accessed=5 * 10**6, transcendentals=0),
        name="gather_weights",
    )(*parts)


def project_kernel(me, column, xs, xa, w_mine, w_other, out, hid):
    n_col = xs.shape[0]
    self_first = me[0] & 1 == 0
    for b in range(xs.shape[1]):
        for n0 in range(0, D, 256):
            total = None
            for k in range(n_col):
                group = (column[0] + n_col - k) & (n_col - 1)
                s, a = xs[group, b], xa[group, b]
                x = jnp.concatenate([jnp.where(self_first, s, a), jnp.where(self_first, a, s)], axis=0)
                w = jnp.concatenate([w_mine[k, n0 : n0 + 256, :], w_other[k, n0 : n0 + 256, :]], axis=1)
                part = jnp.dot(w, x, preferred_element_type=F32)
                total = part if total is None else total + part
            hid[n0 : n0 + 256, :] = jnp.maximum(total, 0.0)
        h = hid[...]
        scale = jnp.sqrt(0.25 + jnp.sum(h * h, axis=0, keepdims=True) / D)
        for j in range(n_col):
            piece = hid[j * ROWS : (j + 1) * ROWS, :] / scale
            out[j, b * ROWS : (b + 1) * ROWS, :] = piece.T.astype(BF)


def project(me, column, xs, xa, w_mine, w_other):
    n_col, n_blk = xs.shape[:2]
    return pl.pallas_call(
        project_kernel,
        out_shape=jax.ShapeDtypeStruct((n_col, n_blk * ROWS, ROWS), BF),
        in_specs=[SMEM] * 2 + [VMEM] * 4,
        out_specs=VMEM,
        scratch_shapes=[pltpu.VMEM((D, ROWS), F32)],
        cost_estimate=pl.CostEstimate(flops=10**9, bytes_accessed=5 * 10**6, transcendentals=0),
        name="project",
    )(me, column, xs, xa, w_mine, w_other)


def body(features, requests, counts, tile_block, local_nbr, tile_count, w_self, w_neigh):
    n_col = lax.axis_size("col")
    me = lax.axis_index("dom").reshape(1).astype(I32)
    column = lax.axis_index("col").reshape(1).astype(I32)
    packed = pack(me, requests[0].T, features)
    sources = [packed[0]]
    for q in range(1, N_SRC):
        sources.append(lax.ppermute(packed[q], "dom", meet_pairs(q // 2, q % 2)))

    todo = plan(me, counts[:, 0], tile_block, tile_count)
    nbr_t, w_t = tables(me, local_nbr, w_self, w_neigh)
    lists, nbrs = [todo], [nbr_t]
    for m in range(1, RING):
        lists.append(lax.ppermute(todo, "dom", ring_pairs(m)))
        nbrs.append(lax.ppermute(nbr_t, "dom", ring_pairs(m)))
    w_all = [w_t]
    for k in range(1, n_col):
        w_all.append(lax.ppermute(w_t, "col", [(i, (i + k) % n_col) for i in range(n_col)]))
    w_mine = gather_weights(w_all)
    w_other = lax.ppermute(w_mine, "dom", [(i, i ^ 1) for i in range(lax.axis_size("dom"))])

    own_parts = own_rows(lists, sources)
    own_here = [own_parts[0]]
    for m in range(1, RING):
        own_here.append(lax.ppermute(own_parts[m], "dom", ring_pairs(RING - m)))
    agg_here = [aggregate(0, lists[0], sources, nbrs[0])]
    for m in range(1, RING):
        part = aggregate(m, lists[m], sources, nbrs[m])
        agg_here.append(lax.ppermute(part, "dom", ring_pairs(RING - m)))

    def to_rows(x):
        return lax.all_to_all(x.reshape(n_col, DST // n_col, ROWS, ROWS), "col", 0, 0, tiled=True)

    xs = to_rows(join(join_own_kernel, (), own_here))
    xa = to_rows(join(join_agg_kernel, (tile_count,), agg_here))
    y = project(me, column, xs, xa, w_mine, w_other)
    return lax.all_to_all(y, "col", 0, 0, tiled=True).reshape(-1, ROWS)


def solution(mesh):
    return jax.shard_map(
        body,
        mesh=mesh,
        in_specs=(
            P("dom", "col"),
            P("dom", None, None),
            P(None, "dom"),
            P("dom", None),
            P("dom", None),
            P("dom"),
            P("col", None),
            P("col", None),
        ),
        out_specs=P("dom", "col"),
        check_vma=False,
    )
```

```python
import jax
import jax.numpy as jnp
from jax import lax
from jax.experimental import pallas as pl
from jax.experimental.pallas import tpu as pltpu
from jax.sharding import PartitionSpec as P


D = 1024
ROWS = 128
CAP = 8
TILES = 32
FAN_T = 4
FRONT = 128
RING = 4
N_SRC = 2 * RING
DST = 16
N_ITEMS = DST * TILES
SECTION = N_ITEMS + ROWS
UNROLL = 4
EARLY = (0, 1, 2, 3, 6, 7)
LATE = (4, 5)
BF = jnp.bfloat16
F32 = jnp.float32
I32 = jnp.int32

VMEM = pl.BlockSpec(memory_space=pltpu.VMEM)
SMEM = pl.BlockSpec(memory_space=pltpu.SMEM)
ANY = pl.BlockSpec(memory_space=pl.ANY)
LIMIT = pltpu.CompilerParams(vmem_limit_bytes=24 * 2**20)


def dom_of(y, x, core):
    return (y * RING + x) * 2 + core


def meet_pairs(d, e):
    pairs = []
    for y in range(RING):
        for x in range(RING):
            for core in range(2):
                if core ^ e == 0:
                    pairs.append((dom_of(y, x, core), dom_of((y + d) % RING, x, 0)))
                else:
                    pairs.append((dom_of(y, x, core), dom_of(y, (x + d) % RING, 1)))
    return pairs


def ring_pairs(m):
    pairs = []
    for y in range(RING):
        for x in range(RING):
            pairs.append((dom_of(y, x, 0), dom_of(y, (x + m) % RING, 0)))
            pairs.append((dom_of(y, x, 1), dom_of((y + m) % RING, x, 1)))
    return pairs


def wrapped(v):
    return lax.rem(v + 2 * RING, RING)


def pack_kernel(me, req, feat, *refs):
    outs, (ft, stage, sem) = refs[:N_SRC], refs[N_SRC:]
    core, x, y = lax.rem(me[0], 2), lax.rem(me[0] // 2, RING), me[0] // (2 * RING)

    def turn(b, _):
        for u in range(8):
            ft[b * 8 + u] = feat[pl.ds((b * 8 + u) * ROWS, ROWS), :].T
        return 0

    lax.fori_loop(0, feat.shape[0] // ROWS // 8, turn, 0)
    copies = []
    for q in range(N_SRC):
        d, e = q // 2, q % 2
        to_one = lax.rem(core + e, 2)
        for m in range(RING):
            shard0 = dom_of(wrapped(y + d), wrapped(x - m), 0)
            shard1 = dom_of(wrapped(y - m), wrapped(x + d), 1)
            shard = jnp.where(to_one == 1, shard1, shard0)
            for s in range(CAP):
                stage[q, m * CAP + s] = ft[req[s, shard]]
        copy = pltpu.make_async_copy(stage.at[q], outs[q], sem.at[q])
        copy.start()
        copies.append(copy)
    for copy in copies:
        copy.wait()


def pack(me, requests, features):
    n_blk = features.shape[0] // ROWS
    return pl.pallas_call(
        pack_kernel,
        out_shape=[jax.ShapeDtypeStruct((RING * CAP, ROWS, ROWS), BF)] * N_SRC,
        in_specs=[SMEM, SMEM, VMEM],
        out_specs=[ANY] * N_SRC,
        scratch_shapes=[
            pltpu.VMEM((n_blk, ROWS, ROWS), BF),
            pltpu.VMEM((N_SRC, RING * CAP, ROWS, ROWS), BF),
            pltpu.SemaphoreType.DMA((N_SRC,)),
        ],
        cost_estimate=pl.CostEstimate(flops=10**9, bytes_accessed=10**7, transcendentals=0),
        compiler_params=LIMIT,
        name="pack",
    )(me, requests, features)


def tables_kernel(me, nbr, ws, wn, nbr_t, w_t):
    half = ROWS // 2

    def turn_nbr(i, _):
        turned = nbr[pl.ds(i * ROWS, ROWS), :].T
        nbr_t[pl.ds(i * half, half), :] = turned[:half] + turned[half:] * 65536
        return 0

    lax.fori_loop(0, nbr.shape[0] // ROWS, turn_nbr, 0, unroll=2)
    for core, w in enumerate((ws, wn)):

        @pl.when(lax.rem(me[0], 2) == core)
        def _():
            for j in range(D // ROWS):
                w_t[j * ROWS : (j + 1) * ROWS, :] = w[:, j * ROWS : (j + 1) * ROWS].T


def tables(me, local_nbr, w_self, w_neigh):
    return pl.pallas_call(
        tables_kernel,
        out_shape=(
            jax.ShapeDtypeStruct((local_nbr.shape[0] // 2, ROWS), I32),
            jax.ShapeDtypeStruct((D, ROWS), BF),
        ),
        in_specs=[SMEM] + [VMEM] * 3,
        out_specs=(VMEM, VMEM),
        cost_estimate=pl.CostEstimate(flops=10**9, bytes_accessed=10**7, transcendentals=0),
        compiler_params=LIMIT,
        name="tables",
    )(me, local_nbr, w_self, w_neigh)


def plan_kernel(me, cnt, tile_block, tile_count, todo, slot, size):
    core, x, y = me[0] & 1, (me[0] >> 1) & (RING - 1), me[0] >> 3
    for m in range(RING):
        size[m] = m * SECTION
        size[RING + m] = m * SECTION + N_ITEMS - 1
    size[2 * RING] = RING * SECTION + SECTION // 2

    def owner(o, p):
        co, xo, yo = o & 1, (o >> 1) & (RING - 1), o >> 3
        q0 = ((y - yo) & (RING - 1)) * 2 + co
        q1 = ((x - xo) & (RING - 1)) * 2 + 1 - co
        q = jnp.where(core == 0, q0, q1)
        m = jnp.where(core == 0, xo - x, yo - y) & (RING - 1)
        first = q * 32 + m * CAP

        def one(s, p):
            slot[p] = first + s
            return p + 1

        return lax.fori_loop(0, cnt[o], one, p)

    lax.fori_loop(0, 2 * RING * RING, owner, jnp.int32(0))

    def block(i, _):
        v = slot[i]
        for m in range(RING):
            todo[m * SECTION + N_ITEMS + 2 + i] = jnp.where((v >> 3) & (RING - 1) == m, v, -1)
        used = tile_count[i]

        def tile(h, _):
            vs = [slot[tile_block[i, h * UNROLL + u]] for u in range(UNROLL)]
            for u, v in enumerate(vs):
                t = h * UNROLL + u
                late = v >> 6 == 2
                m = jnp.where(late, RING, 0) + ((v >> 3) & (RING - 1))
                m = jnp.where(t < used, m, 2 * RING)
                n = size[m]
                todo[n] = v + 256 * i + 4096 * t
                size[m] = n + jnp.where(late, -1, 1)
            return 0

        lax.fori_loop(0, (used + UNROLL - 1) // UNROLL, tile, 0)
        return 0

    lax.fori_loop(0, DST, block, 0)
    for m in range(RING):
        todo[m * SECTION + N_ITEMS] = size[m] - m * SECTION
        todo[m * SECTION + N_ITEMS + 1] = m * SECTION + N_ITEMS - 1 - size[RING + m]


def plan(me, counts, tile_block, tile_count):
    return pl.pallas_call(
        plan_kernel,
        out_shape=jax.ShapeDtypeStruct(((RING + 1) * SECTION,), I32),
        in_specs=[SMEM] * 4,
        out_specs=SMEM,
        scratch_shapes=[pltpu.SMEM((FRONT,), I32), pltpu.SMEM((2 * RING + 1,), I32)],
        cost_estimate=pl.CostEstimate(flops=2 * 10**9, bytes_accessed=10**6, transcendentals=0),
        compiler_params=LIMIT,
        name="plan",
    )(me, counts, tile_block, tile_count)


def own_kernel(*refs):
    lists, src, outs = refs[:RING], refs[RING : RING + N_SRC], refs[RING + N_SRC : 2 * RING + N_SRC]
    stage, sem, sem_out = refs[2 * RING + N_SRC :]

    def copy_of(q, n, v):
        return pltpu.make_async_copy(src[q].at[v & 31], stage.at[n], sem)

    for m in range(RING):

        def start(i, _):
            v = lists[m][m * SECTION + N_ITEMS + 2 + i]

            @pl.when(v >= 0)
            def _():
                for q in range(N_SRC):

                    @pl.when(v >> 5 == q)
                    def _():
                        copy_of(q, m * DST + i, v).start()

            @pl.when(v < 0)
            def _():
                stage[m * DST + i] = jnp.zeros((ROWS, ROWS), BF)

            return 0

        lax.fori_loop(0, DST, start, 0)
    for m in range(RING):

        def finish(i, _):
            @pl.when(lists[m][m * SECTION + N_ITEMS + 2 + i] >= 0)
            def _():
                copy_of(0, 0, 0).wait()

            return 0

        lax.fori_loop(0, DST, finish, 0)
    copies = [
        pltpu.make_async_copy(stage.at[pl.ds(m * DST, DST)], outs[m], sem_out.at[m]) for m in range(RING)
    ]
    for copy in copies:
        copy.start()
    for copy in copies:
        copy.wait()


def own_rows(lists, sources):
    return pl.pallas_call(
        own_kernel,
        out_shape=[jax.ShapeDtypeStruct((DST, ROWS, ROWS), BF)] * RING,
        in_specs=[SMEM] * RING + [ANY] * N_SRC,
        out_specs=[ANY] * RING,
        scratch_shapes=[
            pltpu.VMEM((RING * DST, ROWS, ROWS), BF),
            pltpu.SemaphoreType.DMA,
            pltpu.SemaphoreType.DMA((RING,)),
        ],
        cost_estimate=pl.CostEstimate(flops=10**9, bytes_accessed=10**7, transcendentals=0),
        compiler_params=LIMIT,
        name="own_rows",
    )(*lists, *sources)


def add_sums(lists, nbr, blocks, acc, late):
    iota = lax.broadcasted_iota(I32, (ROWS, ROWS), 0).astype(F32).astype(BF)
    one, zero = jnp.ones((), BF), jnp.zeros((), BF)
    for m in range(RING):
        todo = lists[m]
        n_item = todo[m * SECTION + N_ITEMS + late]

        def some(h, _, m=m, todo=todo, n_item=n_item):
            parts = []
            for u in range(UNROLL):
                n = h * UNROLL + u
                place = m * SECTION + (N_ITEMS - 1 - n if late else n)
                item = jnp.where(n < n_item, todo[place], 128 * late)
                q = (item >> 5) & 7
                q = q - 4 if late else jnp.where(q > 3, q - 2, q)
                blk = q * (RING * CAP) + (item & 31)
                i = (item >> 8) & 15
                t = item >> 12
                row0 = i * (ROWS // 2) + (t & 15) * FAN_T
                shift = (t >> 4) * 16
                total = None
                for f in range(FAN_T):
                    row = (nbr[m][pl.ds(row0 + f, 1), :] >> shift) & 65535
                    hit = jnp.where(iota == row.astype(F32).astype(BF), one, zero)
                    total = hit if total is None else total + hit
                dst = jnp.where(n < n_item, m * DST + i, RING * DST)
                parts.append((dst, jnp.dot(blocks[blk], total, preferred_element_type=F32)))
            for dst, part in parts:
                acc[dst] += part
            return 0

        lax.fori_loop(0, (n_item + UNROLL - 1) // UNROLL, some, 0)


def fetched(src, blocks, sem):
    some = RING * CAP
    copies = [pltpu.make_async_copy(s, blocks.at[pl.ds(q * some, some)], sem.at[q]) for q, s in enumerate(src)]
    for copy in copies:
        copy.start()
    return copies


def early_kernel(*refs):
    lists, src, nbr = refs[:RING], refs[RING : RING + len(EARLY)], refs[RING + len(EARLY) : 2 * RING + len(EARLY)]
    out, blocks, acc, sem, sem_out = refs[2 * RING + len(EARLY) :]
    copies = fetched(src, blocks, sem)

    def clear(n, _):
        acc[n] = jnp.zeros((ROWS, ROWS), F32)
        return 0

    lax.fori_loop(0, RING * DST + 1, clear, 0)
    for copy in copies:
        copy.wait()
    add_sums(lists, nbr, blocks, acc, 0)
    leave = pltpu.make_async_copy(acc.at[pl.ds(0, RING * DST)], out, sem_out)
    leave.start()
    leave.wait()


def early_sums(lists, sources, nbrs):
    return pl.pallas_call(
        early_kernel,
        out_shape=jax.ShapeDtypeStruct((RING * DST, ROWS, ROWS), F32),
        in_specs=[SMEM] * RING + [ANY] * len(EARLY) + [VMEM] * RING,
        out_specs=ANY,
        scratch_shapes=[
            pltpu.VMEM((len(EARLY) * RING * CAP, ROWS, ROWS), BF),
            pltpu.VMEM((RING * DST + 1, ROWS, ROWS), F32),
            pltpu.SemaphoreType.DMA((len(EARLY),)),
            pltpu.SemaphoreType.DMA,
        ],
        cost_estimate=pl.CostEstimate(flops=10**10, bytes_accessed=2 * 10**7, transcendentals=0),
        compiler_params=LIMIT,
        name="early",
    )(*lists, *sources, *nbrs)


def late_kernel(*refs):
    lists, src, nbr = refs[:RING], refs[RING : RING + len(LATE)], refs[RING + len(LATE) : 2 * RING + len(LATE)]
    early, outs = refs[2 * RING + len(LATE)], refs[2 * RING + len(LATE) + 1 : 3 * RING + len(LATE) + 1]
    blocks, acc, sem, sem_in = refs[3 * RING + len(LATE) + 1 :]
    begin = pltpu.make_async_copy(early, acc.at[pl.ds(0, RING * DST)], sem_in)
    begin.start()
    for copy in fetched(src, blocks, sem):
        copy.wait()
    begin.wait()
    add_sums(lists, nbr, blocks, acc, 1)
    for m in range(RING):

        def leave(n, _):
            outs[m][n] = acc[m * DST + n].astype(BF)
            return 0

        lax.fori_loop(0, DST, leave, 0, unroll=4)


def late_sums(lists, sources, nbrs, early):
    return pl.pallas_call(
        late_kernel,
        out_shape=[jax.ShapeDtypeStruct((DST, ROWS, ROWS), BF)] * RING,
        in_specs=[SMEM] * RING + [ANY] * len(LATE) + [VMEM] * RING + [ANY],
        out_specs=[VMEM] * RING,
        scratch_shapes=[
            pltpu.VMEM((len(LATE) * RING * CAP, ROWS, ROWS), BF),
            pltpu.VMEM((RING * DST + 1, ROWS, ROWS), F32),
            pltpu.SemaphoreType.DMA((len(LATE),)),
            pltpu.SemaphoreType.DMA,
        ],
        cost_estimate=pl.CostEstimate(flops=10**10, bytes_accessed=2 * 10**7, transcendentals=0),
        compiler_params=LIMIT,
        name="late",
    )(*lists, *sources, *nbrs, early)


def join_own_kernel(a, b, c, d, out):
    for n in range(DST):
        total = a[n].astype(F32) + b[n].astype(F32) + c[n].astype(F32) + d[n].astype(F32)
        out[n] = total.astype(BF)


def join_agg_kernel(tile_count, a, b, c, d, out):
    for n in range(DST):
        total = a[n].astype(F32) + b[n].astype(F32) + c[n].astype(F32) + d[n].astype(F32)
        out[n] = (total / (tile_count[n] * FAN_T).astype(F32)).astype(BF)


def join(kernel, scalars, parts):
    return pl.pallas_call(
        kernel,
        out_shape=jax.ShapeDtypeStruct((DST, ROWS, ROWS), BF),
        in_specs=[SMEM] * len(scalars) + [VMEM] * RING,
        out_specs=VMEM,
        cost_estimate=pl.CostEstimate(flops=10**9, bytes_accessed=5 * 10**6, transcendentals=0),
        compiler_params=LIMIT,
    )(*scalars, *parts)


def gather_kernel(*refs):
    *parts, out = refs
    for k, part in enumerate(parts):
        out[k] = part[...]


def gather_weights(parts):
    return pl.pallas_call(
        gather_kernel,
        out_shape=jax.ShapeDtypeStruct((len(parts), *parts[0].shape), BF),
        in_specs=[VMEM] * len(parts),
        out_specs=VMEM,
        cost_estimate=pl.CostEstimate(flops=10**9, bytes_accessed=5 * 10**6, transcendentals=0),
        compiler_params=LIMIT,
        name="gather_weights",
    )(*parts)


def project_kernel(me, column, xs, xa, w_mine, w_other, out, hid):
    n_col = xs.shape[0]
    self_first = me[0] & 1 == 0
    for b in range(xs.shape[1]):
        for n0 in range(0, D, 256):
            total = None
            for k in range(n_col):
                group = (column[0] + n_col - k) & (n_col - 1)
                s, a = xs[group, b], xa[group, b]
                x = jnp.concatenate([jnp.where(self_first, s, a), jnp.where(self_first, a, s)], axis=0)
                w = jnp.concatenate([w_mine[k, n0 : n0 + 256, :], w_other[k, n0 : n0 + 256, :]], axis=1)
                part = jnp.dot(w, x, preferred_element_type=F32)
                total = part if total is None else total + part
            hid[n0 : n0 + 256, :] = jnp.maximum(total, 0.0)
        h = hid[...]
        scale = jnp.sqrt(0.25 + jnp.sum(h * h, axis=0, keepdims=True) / D)
        for j in range(n_col):
            piece = hid[j * ROWS : (j + 1) * ROWS, :] / scale
            out[j, b * ROWS : (b + 1) * ROWS, :] = piece.T.astype(BF)


def project(me, column, xs, xa, w_mine, w_other):
    n_col, n_blk = xs.shape[:2]
    return pl.pallas_call(
        project_kernel,
        out_shape=jax.ShapeDtypeStruct((n_col, n_blk * ROWS, ROWS), BF),
        in_specs=[SMEM] * 2 + [VMEM] * 4,
        out_specs=VMEM,
        scratch_shapes=[pltpu.VMEM((D, ROWS), F32)],
        cost_estimate=pl.CostEstimate(flops=10**9, bytes_accessed=5 * 10**6, transcendentals=0),
        compiler_params=LIMIT,
        name="project",
    )(me, column, xs, xa, w_mine, w_other)


def body(features, requests, counts, tile_block, local_nbr, tile_count, w_self, w_neigh):
    n_col = lax.axis_size("col")
    me = lax.axis_index("dom").reshape(1).astype(I32)
    column = lax.axis_index("col").reshape(1).astype(I32)
    packed = pack(me, requests[0].T, features)
    sources = [packed[0]]
    for q in range(1, N_SRC):
        sources.append(lax.ppermute(packed[q], "dom", meet_pairs(q // 2, q % 2)))

    todo = plan(me, counts[:, 0], tile_block, tile_count)
    nbr_t, w_t = tables(me, local_nbr, w_self, w_neigh)
    lists, nbrs = [todo], [nbr_t]
    for m in range(1, RING):
        lists.append(lax.ppermute(todo, "dom", ring_pairs(m)))
        nbrs.append(lax.ppermute(nbr_t, "dom", ring_pairs(m)))
    w_all = [w_t]
    for k in range(1, n_col):
        w_all.append(lax.ppermute(w_t, "col", [(i, (i + k) % n_col) for i in range(n_col)]))
    w_mine = gather_weights(w_all)
    w_other = lax.ppermute(w_mine, "dom", [(i, i ^ 1) for i in range(lax.axis_size("dom"))])

    own_parts = own_rows(lists, sources)
    own_here = [own_parts[0]]
    for m in range(1, RING):
        own_here.append(lax.ppermute(own_parts[m], "dom", ring_pairs(RING - m)))
    early = early_sums(lists, [sources[q] for q in EARLY], nbrs)
    agg_parts = late_sums(lists, [sources[q] for q in LATE], nbrs, early)
    agg_here = [agg_parts[0]]
    for m in range(1, RING):
        agg_here.append(lax.ppermute(agg_parts[m], "dom", ring_pairs(RING - m)))

    def to_rows(x):
        return lax.all_to_all(x.reshape(n_col, DST // n_col, ROWS, ROWS), "col", 0, 0, tiled=True)

    xs = to_rows(join(join_own_kernel, (), own_here))
    xa = to_rows(join(join_agg_kernel, (tile_count,), agg_here))
    y = project(me, column, xs, xa, w_mine, w_other)
    return lax.all_to_all(y, "col", 0, 0, tiled=True).reshape(-1, ROWS)


def solution(mesh):
    return jax.shard_map(
        body,
        mesh=mesh,
        in_specs=(
            P("dom", "col"),
            P("dom", None, None),
            P(None, "dom"),
            P("dom", None),
            P("dom", None),
            P("dom"),
            P("col", None),
            P("col", None),
        ),
        out_specs=P("dom", "col"),
        check_vma=False,
    )
```

```python
import jax
import jax.numpy as jnp
from jax import lax
from jax.experimental import pallas as pl
from jax.experimental.pallas import tpu as pltpu
from jax.sharding import PartitionSpec as P


D = 1024
ROWS = 128
CAP = 8
TILES = 32
FAN_T = 4
FRONT = 128
RING = 4
N_SRC = 2 * RING
DST = 16
N_ITEMS = DST * TILES
SECTION = N_ITEMS + ROWS
UNROLL = 4
EARLY = (0, 1, 2, 3, 6, 7)
LATE = (4, 5)
BF = jnp.bfloat16
F32 = jnp.float32
I32 = jnp.int32

VMEM = pl.BlockSpec(memory_space=pltpu.VMEM)
SMEM = pl.BlockSpec(memory_space=pltpu.SMEM)
ANY = pl.BlockSpec(memory_space=pl.ANY)


def grant(mib):
    return pltpu.CompilerParams(vmem_limit_bytes=mib * 2**20)


LIMIT = grant(8)


def dom_of(y, x, core):
    return (y * RING + x) * 2 + core


def meet_pairs(d, e):
    pairs = []
    for y in range(RING):
        for x in range(RING):
            for core in range(2):
                if core ^ e == 0:
                    pairs.append((dom_of(y, x, core), dom_of((y + d) % RING, x, 0)))
                else:
                    pairs.append((dom_of(y, x, core), dom_of(y, (x + d) % RING, 1)))
    return pairs


def ring_pairs(m):
    pairs = []
    for y in range(RING):
        for x in range(RING):
            pairs.append((dom_of(y, x, 0), dom_of(y, (x + m) % RING, 0)))
            pairs.append((dom_of(y, x, 1), dom_of((y + m) % RING, x, 1)))
    return pairs


def wrapped(v):
    return lax.rem(v + 2 * RING, RING)


def pack_kernel(me, req, feat, *refs):
    outs, (ft, stage, sem) = refs[:N_SRC], refs[N_SRC:]
    core, x, y = lax.rem(me[0], 2), lax.rem(me[0] // 2, RING), me[0] // (2 * RING)

    def turn(b, _):
        for u in range(8):
            ft[b * 8 + u] = feat[pl.ds((b * 8 + u) * ROWS, ROWS), :].T
        return 0

    lax.fori_loop(0, feat.shape[0] // ROWS // 8, turn, 0)
    copies = []
    for q in range(N_SRC):
        d, e = q // 2, q % 2
        to_one = lax.rem(core + e, 2)
        for m in range(RING):
            shard0 = dom_of(wrapped(y + d), wrapped(x - m), 0)
            shard1 = dom_of(wrapped(y - m), wrapped(x + d), 1)
            shard = jnp.where(to_one == 1, shard1, shard0)
            for s in range(CAP):
                stage[q, m * CAP + s] = ft[req[s, shard]]
        copy = pltpu.make_async_copy(stage.at[q], outs[q], sem.at[q])
        copy.start()
        copies.append(copy)
    for copy in copies:
        copy.wait()


def pack(me, requests, features):
    n_blk = features.shape[0] // ROWS
    return pl.pallas_call(
        pack_kernel,
        out_shape=[jax.ShapeDtypeStruct((RING * CAP, ROWS, ROWS), BF)] * N_SRC,
        in_specs=[SMEM, SMEM, VMEM],
        out_specs=[ANY] * N_SRC,
        scratch_shapes=[
            pltpu.VMEM((n_blk, ROWS, ROWS), BF),
            pltpu.VMEM((N_SRC, RING * CAP, ROWS, ROWS), BF),
            pltpu.SemaphoreType.DMA((N_SRC,)),
        ],
        cost_estimate=pl.CostEstimate(flops=10**9, bytes_accessed=10**7, transcendentals=0),
        compiler_params=grant(14),
        name="pack",
    )(me, requests, features)


def tables_kernel(me, nbr, ws, wn, nbr_t, w_t):
    half = ROWS // 2

    def turn_nbr(i, _):
        turned = nbr[pl.ds(i * ROWS, ROWS), :].T
        nbr_t[pl.ds(i * half, half), :] = turned[:half] + turned[half:] * 65536
        return 0

    lax.fori_loop(0, nbr.shape[0] // ROWS, turn_nbr, 0, unroll=2)
    for core, w in enumerate((ws, wn)):

        @pl.when(lax.rem(me[0], 2) == core)
        def _():
            for j in range(D // ROWS):
                w_t[j * ROWS : (j + 1) * ROWS, :] = w[:, j * ROWS : (j + 1) * ROWS].T


def tables(me, local_nbr, w_self, w_neigh):
    return pl.pallas_call(
        tables_kernel,
        out_shape=(
            jax.ShapeDtypeStruct((local_nbr.shape[0] // 2, ROWS), I32),
            jax.ShapeDtypeStruct((D, ROWS), BF),
        ),
        in_specs=[SMEM] + [VMEM] * 3,
        out_specs=(VMEM, VMEM),
        cost_estimate=pl.CostEstimate(flops=10**9, bytes_accessed=10**7, transcendentals=0),
        compiler_params=LIMIT,
        name="tables",
    )(me, local_nbr, w_self, w_neigh)


def plan_kernel(me, cnt, tile_block, tile_count, todo, slot, size):
    core, x, y = me[0] & 1, (me[0] >> 1) & (RING - 1), me[0] >> 3
    for m in range(RING):
        size[m] = m * SECTION
        size[RING + m] = m * SECTION + N_ITEMS - 1
    size[2 * RING] = RING * SECTION + SECTION // 2

    def owner(o, p):
        co, xo, yo = o & 1, (o >> 1) & (RING - 1), o >> 3
        q0 = ((y - yo) & (RING - 1)) * 2 + co
        q1 = ((x - xo) & (RING - 1)) * 2 + 1 - co
        q = jnp.where(core == 0, q0, q1)
        m = jnp.where(core == 0, xo - x, yo - y) & (RING - 1)
        first = q * 32 + m * CAP

        def one(s, p):
            slot[p] = first + s
            return p + 1

        return lax.fori_loop(0, cnt[o], one, p)

    lax.fori_loop(0, 2 * RING * RING, owner, jnp.int32(0))

    def block(i, _):
        v = slot[i]
        for m in range(RING):
            todo[m * SECTION + N_ITEMS + 2 + i] = jnp.where((v >> 3) & (RING - 1) == m, v, -1)
        used = tile_count[i]

        def tile(h, _):
            vs = [slot[tile_block[i, h * UNROLL + u]] for u in range(UNROLL)]
            for u, v in enumerate(vs):
                t = h * UNROLL + u
                late = v >> 6 == 2
                m = jnp.where(late, RING, 0) + ((v >> 3) & (RING - 1))
                m = jnp.where(t < used, m, 2 * RING)
                n = size[m]
                todo[n] = v + 256 * i + 4096 * t
                size[m] = n + jnp.where(late, -1, 1)
            return 0

        lax.fori_loop(0, (used + UNROLL - 1) // UNROLL, tile, 0)
        return 0

    lax.fori_loop(0, DST, block, 0)
    for m in range(RING):
        todo[m * SECTION + N_ITEMS] = size[m] - m * SECTION
        todo[m * SECTION + N_ITEMS + 1] = m * SECTION + N_ITEMS - 1 - size[RING + m]


def plan(me, counts, tile_block, tile_count):
    return pl.pallas_call(
        plan_kernel,
        out_shape=jax.ShapeDtypeStruct(((RING + 1) * SECTION,), I32),
        in_specs=[SMEM] * 4,
        out_specs=SMEM,
        scratch_shapes=[pltpu.SMEM((FRONT,), I32), pltpu.SMEM((2 * RING + 1,), I32)],
        cost_estimate=pl.CostEstimate(flops=2 * 10**9, bytes_accessed=10**6, transcendentals=0),
        compiler_params=LIMIT,
        name="plan",
    )(me, counts, tile_block, tile_count)


def own_kernel(*refs):
    lists, src, outs = refs[:RING], refs[RING : RING + N_SRC], refs[RING + N_SRC : 2 * RING + N_SRC]
    stage, sem, sem_out = refs[2 * RING + N_SRC :]

    def copy_of(q, n, v):
        return pltpu.make_async_copy(src[q].at[v & 31], stage.at[n], sem)

    for m in range(RING):

        def start(i, _):
            v = lists[m][m * SECTION + N_ITEMS + 2 + i]

            @pl.when(v >= 0)
            def _():
                for q in range(N_SRC):

                    @pl.when(v >> 5 == q)
                    def _():
                        copy_of(q, m * DST + i, v).start()

            @pl.when(v < 0)
            def _():
                stage[m * DST + i] = jnp.zeros((ROWS, ROWS), BF)

            return 0

        lax.fori_loop(0, DST, start, 0)
    for m in range(RING):

        def finish(i, _):
            @pl.when(lists[m][m * SECTION + N_ITEMS + 2 + i] >= 0)
            def _():
                copy_of(0, 0, 0).wait()

            return 0

        lax.fori_loop(0, DST, finish, 0)
    copies = [
        pltpu.make_async_copy(stage.at[pl.ds(m * DST, DST)], outs[m], sem_out.at[m]) for m in range(RING)
    ]
    for copy in copies:
        copy.start()
    for copy in copies:
        copy.wait()


def own_rows(lists, sources):
    return pl.pallas_call(
        own_kernel,
        out_shape=[jax.ShapeDtypeStruct((DST, ROWS, ROWS), BF)] * RING,
        in_specs=[SMEM] * RING + [ANY] * N_SRC,
        out_specs=[ANY] * RING,
        scratch_shapes=[
            pltpu.VMEM((RING * DST, ROWS, ROWS), BF),
            pltpu.SemaphoreType.DMA,
            pltpu.SemaphoreType.DMA((RING,)),
        ],
        cost_estimate=pl.CostEstimate(flops=10**9, bytes_accessed=10**7, transcendentals=0),
        compiler_params=LIMIT,
        name="own_rows",
    )(*lists, *sources)


def add_sums(lists, nbr, blocks, acc, late):
    iota = lax.broadcasted_iota(I32, (ROWS, ROWS), 0).astype(F32).astype(BF)
    one, zero = jnp.ones((), BF), jnp.zeros((), BF)
    for m in range(RING):
        todo = lists[m]
        n_item = todo[m * SECTION + N_ITEMS + late]

        def some(h, _, m=m, todo=todo, n_item=n_item):
            parts = []
            for u in range(UNROLL):
                n = h * UNROLL + u
                place = m * SECTION + (N_ITEMS - 1 - n if late else n)
                item = jnp.where(n < n_item, todo[place], 128 * late)
                q = (item >> 5) & 7
                q = q - 4 if late else jnp.where(q > 3, q - 2, q)
                blk = q * (RING * CAP) + (item & 31)
                i = (item >> 8) & 15
                t = item >> 12
                row0 = i * (ROWS // 2) + (t & 15) * FAN_T
                shift = (t >> 4) * 16
                total = None
                for f in range(FAN_T):
                    row = (nbr[m][pl.ds(row0 + f, 1), :] >> shift) & 65535
                    hit = jnp.where(iota == row.astype(F32).astype(BF), one, zero)
                    total = hit if total is None else total + hit
                dst = jnp.where(n < n_item, m * DST + i, RING * DST)
                parts.append((dst, jnp.dot(blocks[blk], total, preferred_element_type=F32)))
            for dst, part in parts:
                acc[dst] += part
            return 0

        lax.fori_loop(0, (n_item + UNROLL - 1) // UNROLL, some, 0)


def fetched(src, blocks, sem):
    some = RING * CAP
    copies = [pltpu.make_async_copy(s, blocks.at[pl.ds(q * some, some)], sem.at[q]) for q, s in enumerate(src)]
    for copy in copies:
        copy.start()
    return copies


def early_kernel(*refs):
    lists, src, nbr = refs[:RING], refs[RING : RING + len(EARLY)], refs[RING + len(EARLY) : 2 * RING + len(EARLY)]
    out, blocks, acc, sem, sem_out = refs[2 * RING + len(EARLY) :]
    copies = fetched(src, blocks, sem)

    def clear(n, _):
        acc[n] = jnp.zeros((ROWS, ROWS), F32)
        return 0

    lax.fori_loop(0, RING * DST + 1, clear, 0)
    for copy in copies:
        copy.wait()
    add_sums(lists, nbr, blocks, acc, 0)
    leave = pltpu.make_async_copy(acc.at[pl.ds(0, RING * DST)], out, sem_out)
    leave.start()
    leave.wait()


def early_sums(lists, sources, nbrs):
    return pl.pallas_call(
        early_kernel,
        out_shape=jax.ShapeDtypeStruct((RING * DST, ROWS, ROWS), F32),
        in_specs=[SMEM] * RING + [ANY] * len(EARLY) + [VMEM] * RING,
        out_specs=ANY,
        scratch_shapes=[
            pltpu.VMEM((len(EARLY) * RING * CAP, ROWS, ROWS), BF),
            pltpu.VMEM((RING * DST + 1, ROWS, ROWS), F32),
            pltpu.SemaphoreType.DMA((len(EARLY),)),
            pltpu.SemaphoreType.DMA,
        ],
        cost_estimate=pl.CostEstimate(flops=10**10, bytes_accessed=2 * 10**7, transcendentals=0),
        compiler_params=grant(15),
        name="early",
    )(*lists, *sources, *nbrs)


def late_kernel(*refs):
    lists, src, nbr = refs[:RING], refs[RING : RING + len(LATE)], refs[RING + len(LATE) : 2 * RING + len(LATE)]
    early, outs = refs[2 * RING + len(LATE)], refs[2 * RING + len(LATE) + 1 : 3 * RING + len(LATE) + 1]
    blocks, acc, sem, sem_in = refs[3 * RING + len(LATE) + 1 :]
    begin = pltpu.make_async_copy(early, acc.at[pl.ds(0, RING * DST)], sem_in)
    begin.start()
    for copy in fetched(src, blocks, sem):
        copy.wait()
    begin.wait()
    add_sums(lists, nbr, blocks, acc, 1)
    for m in range(RING):

        def leave(n, _):
            outs[m][n] = acc[m * DST + n].astype(BF)
            return 0

        lax.fori_loop(0, DST, leave, 0, unroll=4)


def late_sums(lists, sources, nbrs, early):
    return pl.pallas_call(
        late_kernel,
        out_shape=[jax.ShapeDtypeStruct((DST, ROWS, ROWS), BF)] * RING,
        in_specs=[SMEM] * RING + [ANY] * len(LATE) + [VMEM] * RING + [ANY],
        out_specs=[VMEM] * RING,
        scratch_shapes=[
            pltpu.VMEM((len(LATE) * RING * CAP, ROWS, ROWS), BF),
            pltpu.VMEM((RING * DST + 1, ROWS, ROWS), F32),
            pltpu.SemaphoreType.DMA((len(LATE),)),
            pltpu.SemaphoreType.DMA,
        ],
        cost_estimate=pl.CostEstimate(flops=10**10, bytes_accessed=2 * 10**7, transcendentals=0),
        compiler_params=grant(12),
        name="late",
    )(*lists, *sources, *nbrs, early)


def join_own_kernel(a, b, c, d, out):
    for n in range(DST):
        total = a[n].astype(F32) + b[n].astype(F32) + c[n].astype(F32) + d[n].astype(F32)
        out[n] = total.astype(BF)


def join_agg_kernel(tile_count, a, b, c, d, out):
    for n in range(DST):
        total = a[n].astype(F32) + b[n].astype(F32) + c[n].astype(F32) + d[n].astype(F32)
        out[n] = (total / (tile_count[n] * FAN_T).astype(F32)).astype(BF)


def join(kernel, scalars, parts):
    return pl.pallas_call(
        kernel,
        out_shape=jax.ShapeDtypeStruct((DST, ROWS, ROWS), BF),
        in_specs=[SMEM] * len(scalars) + [VMEM] * RING,
        out_specs=VMEM,
        cost_estimate=pl.CostEstimate(flops=10**9, bytes_accessed=5 * 10**6, transcendentals=0),
        compiler_params=LIMIT,
    )(*scalars, *parts)


def gather_kernel(*refs):
    *parts, out = refs
    for k, part in enumerate(parts):
        out[k] = part[...]


def gather_weights(parts):
    return pl.pallas_call(
        gather_kernel,
        out_shape=jax.ShapeDtypeStruct((len(parts), *parts[0].shape), BF),
        in_specs=[VMEM] * len(parts),
        out_specs=VMEM,
        cost_estimate=pl.CostEstimate(flops=10**9, bytes_accessed=5 * 10**6, transcendentals=0),
        compiler_params=LIMIT,
        name="gather_weights",
    )(*parts)


def project_kernel(me, column, xs, xa, w_mine, w_other, out, hid):
    n_col = xs.shape[0]
    self_first = me[0] & 1 == 0
    for b in range(xs.shape[1]):
        for n0 in range(0, D, 256):
            total = None
            for k in range(n_col):
                group = (column[0] + n_col - k) & (n_col - 1)
                s, a = xs[group, b], xa[group, b]
                x = jnp.concatenate([jnp.where(self_first, s, a), jnp.where(self_first, a, s)], axis=0)
                w = jnp.concatenate([w_mine[k, n0 : n0 + 256, :], w_other[k, n0 : n0 + 256, :]], axis=1)
                part = jnp.dot(w, x, preferred_element_type=F32)
                total = part if total is None else total + part
            hid[n0 : n0 + 256, :] = jnp.maximum(total, 0.0)
        h = hid[...]
        scale = jnp.sqrt(0.25 + jnp.sum(h * h, axis=0, keepdims=True) / D)
        for j in range(n_col):
            piece = hid[j * ROWS : (j + 1) * ROWS, :] / scale
            out[j, b * ROWS : (b + 1) * ROWS, :] = piece.T.astype(BF)


def project(me, column, xs, xa, w_mine, w_other):
    n_col, n_blk = xs.shape[:2]
    return pl.pallas_call(
        project_kernel,
        out_shape=jax.ShapeDtypeStruct((n_col, n_blk * ROWS, ROWS), BF),
        in_specs=[SMEM] * 2 + [VMEM] * 4,
        out_specs=VMEM,
        scratch_shapes=[pltpu.VMEM((D, ROWS), F32)],
        cost_estimate=pl.CostEstimate(flops=10**9, bytes_accessed=5 * 10**6, transcendentals=0),
        compiler_params=LIMIT,
        name="project",
    )(me, column, xs, xa, w_mine, w_other)


def body(features, requests, counts, tile_block, local_nbr, tile_count, w_self, w_neigh):
    n_col = lax.axis_size("col")
    me = lax.axis_index("dom").reshape(1).astype(I32)
    column = lax.axis_index("col").reshape(1).astype(I32)
    packed = pack(me, requests[0].T, features)
    sources = [packed[0]]
    for q in range(1, N_SRC):
        sources.append(lax.ppermute(packed[q], "dom", meet_pairs(q // 2, q % 2)))

    todo = plan(me, counts[:, 0], tile_block, tile_count)
    nbr_t, w_t = tables(me, local_nbr, w_self, w_neigh)
    lists, nbrs = [todo], [nbr_t]
    for m in range(1, RING):
        lists.append(lax.ppermute(todo, "dom", ring_pairs(m)))
        nbrs.append(lax.ppermute(nbr_t, "dom", ring_pairs(m)))
    w_all = [w_t]
    for k in range(1, n_col):
        w_all.append(lax.ppermute(w_t, "col", [(i, (i + k) % n_col) for i in range(n_col)]))
    w_mine = gather_weights(w_all)
    w_other = lax.ppermute(w_mine, "dom", [(i, i ^ 1) for i in range(lax.axis_size("dom"))])

    own_parts = own_rows(lists, sources)
    own_here = [own_parts[0]]
    for m in range(1, RING):
        own_here.append(lax.ppermute(own_parts[m], "dom", ring_pairs(RING - m)))
    early = early_sums(lists, [sources[q] for q in EARLY], nbrs)
    agg_parts = late_sums(lists, [sources[q] for q in LATE], nbrs, early)
    agg_here = [agg_parts[0]]
    for m in range(1, RING):
        agg_here.append(lax.ppermute(agg_parts[m], "dom", ring_pairs(RING - m)))

    def to_rows(x):
        return lax.all_to_all(x.reshape(n_col, DST // n_col, ROWS, ROWS), "col", 0, 0, tiled=True)

    xs = to_rows(join(join_own_kernel, (), own_here))
    xa = to_rows(join(join_agg_kernel, (tile_count,), agg_here))
    y = project(me, column, xs, xa, w_mine, w_other)
    return lax.all_to_all(y, "col", 0, 0, tiled=True).reshape(-1, ROWS)


def solution(mesh):
    return jax.shard_map(
        body,
        mesh=mesh,
        in_specs=(
            P("dom", "col"),
            P("dom", None, None),
            P(None, "dom"),
            P("dom", None),
            P("dom", None),
            P("dom"),
            P("col", None),
            P("col", None),
        ),
        out_specs=P("dom", "col"),
        check_vma=False,
    )
```

```python
import jax
import jax.numpy as jnp
from jax import lax
from jax.experimental import pallas as pl
from jax.experimental.pallas import tpu as pltpu
from jax.sharding import PartitionSpec as P


D = 1024
ROWS = 128
CAP = 8
TILES = 32
FAN_T = 4
FRONT = 128
RING = 4
N_SRC = 2 * RING
DST = 16
N_COL = 8
ROW_BLK = DST // N_COL
N_ITEMS = DST * TILES
SECTION = N_ITEMS + ROWS
UNROLL = 4
EARLY = (0, 1, 2, 3, 6, 7)
LATE = (4, 5)
BF = jnp.bfloat16
F32 = jnp.float32
I32 = jnp.int32

VMEM = pl.BlockSpec(memory_space=pltpu.VMEM)
SMEM = pl.BlockSpec(memory_space=pltpu.SMEM)
ANY = pl.BlockSpec(memory_space=pl.ANY)


def grant(mib):
    return pltpu.CompilerParams(vmem_limit_bytes=mib * 2**20)


LIMIT = grant(8)


def dom_of(y, x, core):
    return (y * RING + x) * 2 + core


def meet_pairs(d, e):
    pairs = []
    for y in range(RING):
        for x in range(RING):
            for core in range(2):
                if core ^ e == 0:
                    pairs.append((dom_of(y, x, core), dom_of((y + d) % RING, x, 0)))
                else:
                    pairs.append((dom_of(y, x, core), dom_of(y, (x + d) % RING, 1)))
    return pairs


def ring_pairs(m):
    pairs = []
    for y in range(RING):
        for x in range(RING):
            pairs.append((dom_of(y, x, 0), dom_of(y, (x + m) % RING, 0)))
            pairs.append((dom_of(y, x, 1), dom_of((y + m) % RING, x, 1)))
    return pairs


def col_pairs(k):
    return [(i, (i + k) % N_COL) for i in range(N_COL)]


def wrapped(v):
    return lax.rem(v + 2 * RING, RING)


def pack_kernel(me, req, feat, *refs):
    outs, (ft, stage, sem) = refs[:N_SRC], refs[N_SRC:]
    core, x, y = lax.rem(me[0], 2), lax.rem(me[0] // 2, RING), me[0] // (2 * RING)

    def turn(b, _):
        for u in range(8):
            ft[b * 8 + u] = feat[pl.ds((b * 8 + u) * ROWS, ROWS), :].T
        return 0

    lax.fori_loop(0, feat.shape[0] // ROWS // 8, turn, 0)
    copies = []
    for q in range(N_SRC):
        d, e = q // 2, q % 2
        to_one = lax.rem(core + e, 2)
        for m in range(RING):
            shard0 = dom_of(wrapped(y + d), wrapped(x - m), 0)
            shard1 = dom_of(wrapped(y - m), wrapped(x + d), 1)
            shard = jnp.where(to_one == 1, shard1, shard0)
            for s in range(CAP):
                stage[q, m * CAP + s] = ft[req[s, shard]]
        copy = pltpu.make_async_copy(stage.at[q], outs[q], sem.at[q])
        copy.start()
        copies.append(copy)
    for copy in copies:
        copy.wait()


def pack(me, requests, features):
    n_blk = features.shape[0] // ROWS
    return pl.pallas_call(
        pack_kernel,
        out_shape=[jax.ShapeDtypeStruct((RING * CAP, ROWS, ROWS), BF)] * N_SRC,
        in_specs=[SMEM, SMEM, VMEM],
        out_specs=[ANY] * N_SRC,
        scratch_shapes=[
            pltpu.VMEM((n_blk, ROWS, ROWS), BF),
            pltpu.VMEM((N_SRC, RING * CAP, ROWS, ROWS), BF),
            pltpu.SemaphoreType.DMA((N_SRC,)),
        ],
        cost_estimate=pl.CostEstimate(flops=10**9, bytes_accessed=10**7, transcendentals=0),
        compiler_params=grant(14),
        name="pack",
    )(me, requests, features)


def turn_nbr_kernel(nbr, out):
    half = ROWS // 2
    for i in range(nbr.shape[0] // ROWS):
        turned = nbr[i * ROWS : (i + 1) * ROWS, :].T
        out[i * half : (i + 1) * half, :] = turned[:half] + turned[half:] * 65536


def turn_nbr(local_nbr):
    some = 4 * ROWS
    return pl.pallas_call(
        turn_nbr_kernel,
        grid=(local_nbr.shape[0] // some,),
        out_shape=jax.ShapeDtypeStruct((local_nbr.shape[0] // 2, ROWS), I32),
        in_specs=[pl.BlockSpec((some, ROWS), lambda g: (g, 0))],
        out_specs=pl.BlockSpec((some // 2, ROWS), lambda g: (g, 0)),
        cost_estimate=pl.CostEstimate(flops=10**9, bytes_accessed=10**7, transcendentals=0),
        compiler_params=LIMIT,
        name="turn_nbr",
    )(local_nbr)


def turn_weights_kernel(me, ws, wn, w_t):
    for core, w in enumerate((ws, wn)):

        @pl.when(me[0] & 1 == core)
        def _():
            for j in range(D // ROWS):
                w_t[j * ROWS : (j + 1) * ROWS, :] = w[:, j * ROWS : (j + 1) * ROWS].T


def turn_weights(me, w_self, w_neigh):
    return pl.pallas_call(
        turn_weights_kernel,
        out_shape=jax.ShapeDtypeStruct((D, ROWS), BF),
        in_specs=[SMEM] + [VMEM] * 2,
        out_specs=VMEM,
        cost_estimate=pl.CostEstimate(flops=10**9, bytes_accessed=10**7, transcendentals=0),
        compiler_params=LIMIT,
        name="turn_weights",
    )(me, w_self, w_neigh)


def plan_kernel(me, cnt, tile_block, tile_count, todo, slot, size):
    core, x, y = me[0] & 1, (me[0] >> 1) & (RING - 1), me[0] >> 3
    for m in range(RING):
        size[m] = m * SECTION
        size[RING + m] = m * SECTION + N_ITEMS - 1
    size[2 * RING] = RING * SECTION + SECTION // 2

    def owner(o, p):
        co, xo, yo = o & 1, (o >> 1) & (RING - 1), o >> 3
        q0 = ((y - yo) & (RING - 1)) * 2 + co
        q1 = ((x - xo) & (RING - 1)) * 2 + 1 - co
        q = jnp.where(core == 0, q0, q1)
        m = jnp.where(core == 0, xo - x, yo - y) & (RING - 1)
        first = q * 32 + m * CAP

        def one(s, p):
            slot[p] = first + s
            return p + 1

        return lax.fori_loop(0, cnt[o], one, p)

    lax.fori_loop(0, 2 * RING * RING, owner, jnp.int32(0))

    def block(i, _):
        v = slot[i]
        for m in range(RING):
            todo[m * SECTION + N_ITEMS + 2 + i] = jnp.where((v >> 3) & (RING - 1) == m, v, -1)
        used = tile_count[i]

        def tile(h, _):
            vs = [slot[tile_block[i, h * UNROLL + u]] for u in range(UNROLL)]
            for u, v in enumerate(vs):
                t = h * UNROLL + u
                late = v >> 6 == 2
                m = jnp.where(late, RING, 0) + ((v >> 3) & (RING - 1))
                m = jnp.where(t < used, m, 2 * RING)
                n = size[m]
                todo[n] = v + 256 * i + 4096 * t
                size[m] = n + jnp.where(late, -1, 1)
            return 0

        lax.fori_loop(0, (used + UNROLL - 1) // UNROLL, tile, 0)
        return 0

    lax.fori_loop(0, DST, block, 0)
    for m in range(RING):
        todo[m * SECTION + N_ITEMS] = size[m] - m * SECTION
        todo[m * SECTION + N_ITEMS + 1] = m * SECTION + N_ITEMS - 1 - size[RING + m]


def plan(me, counts, tile_block, tile_count):
    return pl.pallas_call(
        plan_kernel,
        out_shape=jax.ShapeDtypeStruct(((RING + 1) * SECTION,), I32),
        in_specs=[SMEM] * 4,
        out_specs=SMEM,
        scratch_shapes=[pltpu.SMEM((FRONT,), I32), pltpu.SMEM((2 * RING + 1,), I32)],
        cost_estimate=pl.CostEstimate(flops=2 * 10**9, bytes_accessed=10**6, transcendentals=0),
        compiler_params=LIMIT,
        name="plan",
    )(me, counts, tile_block, tile_count)


def own_kernel(*refs):
    lists, src, outs = refs[:RING], refs[RING : RING + N_SRC], refs[RING + N_SRC :]
    for m in range(RING):

        def place(i, _, m=m):
            v = lists[m][m * SECTION + N_ITEMS + 2 + i]

            @pl.when(v < 0)
            def _():
                outs[m][i] = jnp.zeros((ROWS, ROWS), BF)

            @pl.when(v >= 0)
            def _():
                for q in range(N_SRC):

                    @pl.when(v >> 5 == q)
                    def _():
                        outs[m][i] = src[q][v & 31]

            return 0

        lax.fori_loop(0, DST, place, 0)


def own_rows(lists, sources):
    return pl.pallas_call(
        own_kernel,
        out_shape=[jax.ShapeDtypeStruct((DST, ROWS, ROWS), BF)] * RING,
        in_specs=[SMEM] * RING + [VMEM] * N_SRC,
        out_specs=[VMEM] * RING,
        cost_estimate=pl.CostEstimate(flops=10**9, bytes_accessed=10**7, transcendentals=0),
        compiler_params=grant(12),
        name="own_rows",
    )(*lists, *sources)


def add_sums(lists, nbr, block_of, acc, late):
    iota = lax.broadcasted_iota(I32, (ROWS, ROWS), 0).astype(F32).astype(BF)
    one, zero = jnp.ones((), BF), jnp.zeros((), BF)
    for m in range(RING):
        todo = lists[m]
        n_item = todo[m * SECTION + N_ITEMS + late]

        def some(h, _, m=m, todo=todo, n_item=n_item):
            parts = []
            for u in range(UNROLL):
                n = h * UNROLL + u
                place = m * SECTION + (N_ITEMS - 1 - n if late else n)
                item = jnp.where(n < n_item, todo[place], 128 * late)
                block = block_of((item >> 5) & 7, item & 31)
                i = (item >> 8) & 15
                t = item >> 12
                row0 = i * (ROWS // 2) + (t & 15) * FAN_T
                shift = (t >> 4) * 16
                total = None
                for f in range(FAN_T):
                    row = (nbr[m][pl.ds(row0 + f, 1), :] >> shift) & 65535
                    hit = jnp.where(iota == row.astype(F32).astype(BF), one, zero)
                    total = hit if total is None else total + hit
                dst = jnp.where(n < n_item, m * DST + i, RING * DST)
                parts.append((dst, jnp.dot(block, total, preferred_element_type=F32)))
            for dst, part in parts:
                acc[dst] += part
            return 0

        lax.fori_loop(0, (n_item + UNROLL - 1) // UNROLL, some, 0)


def fetched(src, blocks, sem):
    some = RING * CAP
    copies = [pltpu.make_async_copy(s, blocks.at[pl.ds(q * some, some)], sem.at[q]) for q, s in enumerate(src)]
    for copy in copies:
        copy.start()
    return copies


def early_kernel(*refs):
    lists, src, nbr = refs[:RING], refs[RING : RING + len(EARLY)], refs[RING + len(EARLY) : 2 * RING + len(EARLY)]
    acc, blocks, sem = refs[2 * RING + len(EARLY) :]
    copies = fetched(src, blocks, sem)

    def clear(n, _):
        acc[n] = jnp.zeros((ROWS, ROWS), F32)
        return 0

    lax.fori_loop(0, RING * DST + 1, clear, 0)
    for copy in copies:
        copy.wait()

    def block_of(q, b):
        return blocks[jnp.where(q > 3, q - 2, q) * (RING * CAP) + b]

    add_sums(lists, nbr, block_of, acc, 0)


def early_sums(lists, sources, nbrs):
    return pl.pallas_call(
        early_kernel,
        out_shape=jax.ShapeDtypeStruct((RING * DST + 1, ROWS, ROWS), F32),
        in_specs=[SMEM] * RING + [ANY] * len(EARLY) + [VMEM] * RING,
        out_specs=VMEM,
        scratch_shapes=[
            pltpu.VMEM((len(EARLY) * RING * CAP, ROWS, ROWS), BF),
            pltpu.SemaphoreType.DMA((len(EARLY),)),
        ],
        cost_estimate=pl.CostEstimate(flops=10**10, bytes_accessed=2 * 10**7, transcendentals=0),
        compiler_params=grant(15),
        name="early",
    )(*lists, *sources, *nbrs)


def late_kernel(*refs):
    lists, src, nbr = refs[:RING], refs[RING : RING + len(LATE)], refs[RING + len(LATE) : 2 * RING + len(LATE)]
    _, *outs, acc = refs[2 * RING + len(LATE) :]

    def block_of(q, b):
        return jnp.where(q == LATE[0], src[0][b], src[1][b])

    add_sums(lists, nbr, block_of, acc, 1)
    for m in range(RING):

        def leave(n, _, m=m):
            outs[m][n] = acc[m * DST + n].astype(BF)
            return 0

        lax.fori_loop(0, DST, leave, 0, unroll=4)


def late_sums(lists, sources, nbrs, early):
    n_in = 2 * RING + len(LATE)
    return pl.pallas_call(
        late_kernel,
        out_shape=[jax.ShapeDtypeStruct((DST, ROWS, ROWS), BF)] * RING + [jax.ShapeDtypeStruct(early.shape, F32)],
        in_specs=[SMEM] * RING + [VMEM] * (len(LATE) + RING + 1),
        out_specs=[VMEM] * (RING + 1),
        input_output_aliases={n_in: RING},
        cost_estimate=pl.CostEstimate(flops=10**10, bytes_accessed=2 * 10**7, transcendentals=0),
        compiler_params=grant(12),
        name="late",
    )(*lists, *sources, *nbrs, early)[:RING]


def join_own_kernel(a, b, c, d, out):
    for n in range(DST):
        out[n] = (a[n].astype(F32) + b[n].astype(F32) + c[n].astype(F32) + d[n].astype(F32)).astype(BF)


def join_agg_kernel(column, tile_count, a, b, c, d, *outs):
    for k, out in enumerate(outs):
        for j in range(ROW_BLK):
            n = ((column[0] + k) & (N_COL - 1)) * ROW_BLK + j
            total = a[n].astype(F32) + b[n].astype(F32) + c[n].astype(F32) + d[n].astype(F32)
            out[j] = (total / (tile_count[n] * FAN_T).astype(F32)).astype(BF)


def join(kernel, scalars, parts, shapes):
    return pl.pallas_call(
        kernel,
        out_shape=[jax.ShapeDtypeStruct(shape, BF) for shape in shapes],
        in_specs=[SMEM] * len(scalars) + [VMEM] * RING,
        out_specs=[VMEM] * len(shapes),
        cost_estimate=pl.CostEstimate(flops=10**9, bytes_accessed=5 * 10**6, transcendentals=0),
        compiler_params=LIMIT,
    )(*scalars, *parts)


def gather_kernel(*refs):
    *parts, out = refs
    for k, part in enumerate(parts):
        out[k] = part[...]


def gather_weights(parts):
    return pl.pallas_call(
        gather_kernel,
        out_shape=jax.ShapeDtypeStruct((len(parts), *parts[0].shape), BF),
        in_specs=[VMEM] * len(parts),
        out_specs=VMEM,
        cost_estimate=pl.CostEstimate(flops=10**9, bytes_accessed=5 * 10**6, transcendentals=0),
        compiler_params=LIMIT,
        name="gather_weights",
    )(*parts)


def project_kernel(me, column, xs, *refs):
    xa, (w_mine, w_other, out, hid) = refs[:N_COL], refs[N_COL:]
    self_first = me[0] & 1 == 0
    for b in range(ROW_BLK):
        for n0 in range(0, D, 256):
            total = None
            for k in range(N_COL):
                s, a = xs[(column[0] - k) & (N_COL - 1), b], xa[k][b]
                x = jnp.concatenate([jnp.where(self_first, s, a), jnp.where(self_first, a, s)], axis=0)
                w = jnp.concatenate([w_mine[k, n0 : n0 + 256, :], w_other[k, n0 : n0 + 256, :]], axis=1)
                part = jnp.dot(w, x, preferred_element_type=F32)
                total = part if total is None else total + part
            hid[n0 : n0 + 256, :] = jnp.maximum(total, 0.0)
        h = hid[...]
        scale = jnp.sqrt(0.25 + jnp.sum(h * h, axis=0, keepdims=True) / D)
        for j in range(N_COL):
            piece = hid[j * ROWS : (j + 1) * ROWS, :] / scale
            out[j, b * ROWS : (b + 1) * ROWS, :] = piece.T.astype(BF)


def project(me, column, xs, xa, w_mine, w_other):
    return pl.pallas_call(
        project_kernel,
        out_shape=jax.ShapeDtypeStruct((N_COL, ROW_BLK * ROWS, ROWS), BF),
        in_specs=[SMEM] * 2 + [VMEM] * (N_COL + 3),
        out_specs=VMEM,
        scratch_shapes=[pltpu.VMEM((D, ROWS), F32)],
        cost_estimate=pl.CostEstimate(flops=10**9, bytes_accessed=5 * 10**6, transcendentals=0),
        compiler_params=LIMIT,
        name="project",
    )(me, column, xs, *xa, w_mine, w_other)


def body(features, requests, counts, tile_block, local_nbr, tile_count, w_self, w_neigh):
    me = lax.axis_index("dom").reshape(1).astype(I32)
    column = lax.axis_index("col").reshape(1).astype(I32)
    packed = pack(me, requests[0].T, features)
    sources = [packed[0]]
    for q in range(1, N_SRC):
        sources.append(lax.ppermute(packed[q], "dom", meet_pairs(q // 2, q % 2)))

    todo = plan(me, counts[:, 0], tile_block, tile_count)
    nbr_t = turn_nbr(local_nbr)
    w_t = turn_weights(me, w_self, w_neigh)
    lists, nbrs = [todo], [nbr_t]
    for m in range(1, RING):
        lists.append(lax.ppermute(todo, "dom", ring_pairs(m)))
        nbrs.append(lax.ppermute(nbr_t, "dom", ring_pairs(m)))
    w_all = [w_t]
    for k in range(1, N_COL):
        w_all.append(lax.ppermute(w_t, "col", col_pairs(k)))
    w_mine = gather_weights(w_all)
    w_other = lax.ppermute(w_mine, "dom", [(i, i ^ 1) for i in range(lax.axis_size("dom"))])

    own_parts = own_rows(lists, sources)
    own_here = [own_parts[0]]
    for m in range(1, RING):
        own_here.append(lax.ppermute(own_parts[m], "dom", ring_pairs(RING - m)))
    early = early_sums(lists, [sources[q] for q in EARLY], nbrs)
    agg_parts = late_sums(lists, [sources[q] for q in LATE], nbrs, early)
    agg_here = [agg_parts[0]]
    for m in range(1, RING):
        agg_here.append(lax.ppermute(agg_parts[m], "dom", ring_pairs(RING - m)))

    (own_sum,) = join(join_own_kernel, (), own_here, [(DST, ROWS, ROWS)])
    xs = lax.all_to_all(own_sum.reshape(N_COL, ROW_BLK, ROWS, ROWS), "col", 0, 0, tiled=True)
    parts = join(join_agg_kernel, (column, tile_count), agg_here, [(ROW_BLK, ROWS, ROWS)] * N_COL)
    xa = [parts[0]] + [lax.ppermute(parts[k], "col", col_pairs(k)) for k in range(1, N_COL)]
    y = project(me, column, xs, xa, w_mine, w_other)
    return lax.all_to_all(y, "col", 0, 0, tiled=True).reshape(-1, ROWS)


def solution(mesh):
    return jax.shard_map(
        body,
        mesh=mesh,
        in_specs=(
            P("dom", "col"),
            P("dom", None, None),
            P(None, "dom"),
            P("dom", None),
            P("dom", None),
            P("dom"),
            P("col", None),
            P("col", None),
        ),
        out_specs=P("dom", "col"),
        check_vma=False,
    )
```

```python
import jax
import jax.numpy as jnp
from jax import lax
from jax.experimental import pallas as pl
from jax.experimental.pallas import tpu as pltpu
from jax.sharding import PartitionSpec as P


D = 1024
ROWS = 128
CAP = 8
TILES = 32
FAN_T = 4
FRONT = 128
RING = 4
N_SRC = 2 * RING
DST = 16
N_COL = 8
ROW_BLK = DST // N_COL
N_ITEMS = DST * TILES
SECTION = N_ITEMS + ROWS
UNROLL = 4
EARLY = (0, 1, 2, 3, 6, 7)
LATE = (4, 5)
BF = jnp.bfloat16
F32 = jnp.float32
I32 = jnp.int32

VMEM = pl.BlockSpec(memory_space=pltpu.VMEM)
SMEM = pl.BlockSpec(memory_space=pltpu.SMEM)
ANY = pl.BlockSpec(memory_space=pl.ANY)


def grant(mib):
    return pltpu.CompilerParams(vmem_limit_bytes=mib * 2**20)


LIMIT = grant(8)


def dom_of(y, x, core):
    return (y * RING + x) * 2 + core


def meet_pairs(d, e):
    pairs = []
    for y in range(RING):
        for x in range(RING):
            for core in range(2):
                if core ^ e == 0:
                    pairs.append((dom_of(y, x, core), dom_of((y + d) % RING, x, 0)))
                else:
                    pairs.append((dom_of(y, x, core), dom_of(y, (x + d) % RING, 1)))
    return pairs


def ring_pairs(m):
    pairs = []
    for y in range(RING):
        for x in range(RING):
            pairs.append((dom_of(y, x, 0), dom_of(y, (x + m) % RING, 0)))
            pairs.append((dom_of(y, x, 1), dom_of((y + m) % RING, x, 1)))
    return pairs


def col_pairs(k):
    return [(i, (i + k) % N_COL) for i in range(N_COL)]


def wrapped(v):
    return lax.rem(v + 2 * RING, RING)


def pack_kernel(me, req, feat, *refs):
    outs, (ft, stage, sem) = refs[:N_SRC], refs[N_SRC:]
    core, x, y = lax.rem(me[0], 2), lax.rem(me[0] // 2, RING), me[0] // (2 * RING)

    def turn(b, _):
        for u in range(8):
            ft[b * 8 + u] = feat[pl.ds((b * 8 + u) * ROWS, ROWS), :].T
        return 0

    lax.fori_loop(0, feat.shape[0] // ROWS // 8, turn, 0)
    copies = []
    for q in range(N_SRC):
        d, e = q // 2, q % 2
        to_one = lax.rem(core + e, 2)
        for m in range(RING):
            shard0 = dom_of(wrapped(y + d), wrapped(x - m), 0)
            shard1 = dom_of(wrapped(y - m), wrapped(x + d), 1)
            shard = jnp.where(to_one == 1, shard1, shard0)
            for s in range(CAP):
                stage[q, m * CAP + s] = ft[req[s, shard]]
        copy = pltpu.make_async_copy(stage.at[q], outs[q], sem.at[q])
        copy.start()
        copies.append(copy)
    for copy in copies:
        copy.wait()


def pack(me, requests, features):
    n_blk = features.shape[0] // ROWS
    return pl.pallas_call(
        pack_kernel,
        out_shape=[jax.ShapeDtypeStruct((RING * CAP, ROWS, ROWS), BF)] * N_SRC,
        in_specs=[SMEM, SMEM, VMEM],
        out_specs=[ANY] * N_SRC,
        scratch_shapes=[
            pltpu.VMEM((n_blk, ROWS, ROWS), BF),
            pltpu.VMEM((N_SRC, RING * CAP, ROWS, ROWS), BF),
            pltpu.SemaphoreType.DMA((N_SRC,)),
        ],
        cost_estimate=pl.CostEstimate(flops=10**9, bytes_accessed=10**7, transcendentals=0),
        compiler_params=grant(14),
        name="pack",
    )(me, requests, features)


def turn_nbr_kernel(nbr, out):
    half = ROWS // 2
    for i in range(nbr.shape[0] // ROWS):
        turned = nbr[i * ROWS : (i + 1) * ROWS, :].T
        out[i * half : (i + 1) * half, :] = turned[:half] + turned[half:] * 65536


def turn_nbr(local_nbr):
    some = 4 * ROWS
    return pl.pallas_call(
        turn_nbr_kernel,
        grid=(local_nbr.shape[0] // some,),
        out_shape=jax.ShapeDtypeStruct((local_nbr.shape[0] // 2, ROWS), I32),
        in_specs=[pl.BlockSpec((some, ROWS), lambda g: (g, 0))],
        out_specs=pl.BlockSpec((some // 2, ROWS), lambda g: (g, 0)),
        cost_estimate=pl.CostEstimate(flops=10**9, bytes_accessed=10**7, transcendentals=0),
        compiler_params=LIMIT,
        name="turn_nbr",
    )(local_nbr)


def turn_weights_kernel(me, ws, wn, w_t):
    for core, w in enumerate((ws, wn)):

        @pl.when(me[0] & 1 == core)
        def _():
            for j in range(D // ROWS):
                w_t[j * ROWS : (j + 1) * ROWS, :] = w[:, j * ROWS : (j + 1) * ROWS].T


def turn_weights(me, w_self, w_neigh):
    return pl.pallas_call(
        turn_weights_kernel,
        out_shape=jax.ShapeDtypeStruct((D, ROWS), BF),
        in_specs=[SMEM] + [VMEM] * 2,
        out_specs=VMEM,
        cost_estimate=pl.CostEstimate(flops=10**9, bytes_accessed=10**7, transcendentals=0),
        compiler_params=LIMIT,
        name="turn_weights",
    )(me, w_self, w_neigh)


def plan_kernel(me, cnt, tile_block, tile_count, todo, slot, size):
    core, x, y = me[0] & 1, (me[0] >> 1) & (RING - 1), me[0] >> 3
    for m in range(RING):
        size[m] = m * SECTION
        size[RING + m] = m * SECTION + N_ITEMS - 1
    size[2 * RING] = RING * SECTION + SECTION // 2

    def owner(o, p):
        co, xo, yo = o & 1, (o >> 1) & (RING - 1), o >> 3
        q0 = ((y - yo) & (RING - 1)) * 2 + co
        q1 = ((x - xo) & (RING - 1)) * 2 + 1 - co
        q = jnp.where(core == 0, q0, q1)
        m = jnp.where(core == 0, xo - x, yo - y) & (RING - 1)
        first = q * 32 + m * CAP

        def one(s, p):
            slot[p] = first + s
            return p + 1

        return lax.fori_loop(0, cnt[o], one, p)

    lax.fori_loop(0, 2 * RING * RING, owner, jnp.int32(0))

    def block(i, _):
        v = slot[i]
        for m in range(RING):
            todo[m * SECTION + N_ITEMS + 2 + i] = jnp.where((v >> 3) & (RING - 1) == m, v, -1)
        used = tile_count[i]

        def tile(h, _):
            vs = [slot[tile_block[i, h * UNROLL + u]] for u in range(UNROLL)]
            for u, v in enumerate(vs):
                t = h * UNROLL + u
                late = v >> 6 == 2
                m = jnp.where(late, RING, 0) + ((v >> 3) & (RING - 1))
                m = jnp.where(t < used, m, 2 * RING)
                n = size[m]
                todo[n] = v + 256 * i + 4096 * t
                size[m] = n + jnp.where(late, -1, 1)
            return 0

        lax.fori_loop(0, (used + UNROLL - 1) // UNROLL, tile, 0)
        return 0

    lax.fori_loop(0, DST, block, 0)
    for m in range(RING):
        todo[m * SECTION + N_ITEMS] = size[m] - m * SECTION
        todo[m * SECTION + N_ITEMS + 1] = m * SECTION + N_ITEMS - 1 - size[RING + m]


def plan(me, counts, tile_block, tile_count):
    return pl.pallas_call(
        plan_kernel,
        out_shape=jax.ShapeDtypeStruct(((RING + 1) * SECTION,), I32),
        in_specs=[SMEM] * 4,
        out_specs=SMEM,
        scratch_shapes=[pltpu.SMEM((FRONT,), I32), pltpu.SMEM((2 * RING + 1,), I32)],
        cost_estimate=pl.CostEstimate(flops=2 * 10**9, bytes_accessed=10**6, transcendentals=0),
        compiler_params=LIMIT,
        name="plan",
    )(me, counts, tile_block, tile_count)


def own_kernel(*refs):
    lists, src, outs = refs[:RING], refs[RING : RING + N_SRC], refs[RING + N_SRC :]
    for m in range(RING):

        def place(i, _, m=m):
            v = lists[m][m * SECTION + N_ITEMS + 2 + i]

            @pl.when(v < 0)
            def _():
                outs[m][i] = jnp.zeros((ROWS, ROWS), BF)

            @pl.when(v >= 0)
            def _():
                for q in range(N_SRC):

                    @pl.when(v >> 5 == q)
                    def _():
                        outs[m][i] = src[q][v & 31]

            return 0

        lax.fori_loop(0, DST, place, 0)


def own_rows(lists, sources):
    return pl.pallas_call(
        own_kernel,
        out_shape=[jax.ShapeDtypeStruct((DST, ROWS, ROWS), BF)] * RING,
        in_specs=[SMEM] * RING + [VMEM] * N_SRC,
        out_specs=[VMEM] * RING,
        cost_estimate=pl.CostEstimate(flops=10**9, bytes_accessed=10**7, transcendentals=0),
        compiler_params=grant(12),
        name="own_rows",
    )(*lists, *sources)


def add_sums(lists, nbr, block_of, acc, late):
    iota = lax.broadcasted_iota(I32, (ROWS, ROWS), 0).astype(F32).astype(BF)
    one, zero = jnp.ones((), BF), jnp.zeros((), BF)
    for m in range(RING):
        todo = lists[m]
        n_item = todo[m * SECTION + N_ITEMS + late]

        def some(h, _, m=m, todo=todo, n_item=n_item):
            parts = []
            for u in range(UNROLL):
                n = h * UNROLL + u
                place = m * SECTION + (N_ITEMS - 1 - n if late else n)
                item = jnp.where(n < n_item, todo[place], 128 * late)
                block = block_of((item >> 5) & 7, item & 31)
                i = (item >> 8) & 15
                t = item >> 12
                row0 = i * (ROWS // 2) + (t & 15) * FAN_T
                shift = (t >> 4) * 16
                total = None
                for f in range(FAN_T):
                    row = (nbr[m][pl.ds(row0 + f, 1), :] >> shift) & 65535
                    hit = jnp.where(iota == row.astype(F32).astype(BF), one, zero)
                    total = hit if total is None else total + hit
                dst = jnp.where(n < n_item, m * DST + i, RING * DST)
                parts.append((dst, jnp.dot(block, total, preferred_element_type=F32)))
            for dst, part in parts:
                acc[dst] += part
            return 0

        lax.fori_loop(0, (n_item + UNROLL - 1) // UNROLL, some, 0)


def fetched(src, blocks, sem):
    some = RING * CAP
    copies = [pltpu.make_async_copy(s, blocks.at[pl.ds(q * some, some)], sem.at[q]) for q, s in enumerate(src)]
    for copy in copies:
        copy.start()
    return copies


def early_kernel(*refs):
    lists, src, nbr = refs[:RING], refs[RING : RING + len(EARLY)], refs[RING + len(EARLY) : 2 * RING + len(EARLY)]
    acc, blocks, sem = refs[2 * RING + len(EARLY) :]
    copies = fetched(src, blocks, sem)

    def clear(n, _):
        acc[n] = jnp.zeros((ROWS, ROWS), F32)
        return 0

    lax.fori_loop(0, RING * DST + 1, clear, 0)
    for copy in copies:
        copy.wait()

    def block_of(q, b):
        return blocks[jnp.where(q > 3, q - 2, q) * (RING * CAP) + b]

    add_sums(lists, nbr, block_of, acc, 0)


def early_sums(lists, sources, nbrs):
    return pl.pallas_call(
        early_kernel,
        out_shape=jax.ShapeDtypeStruct((RING * DST + 1, ROWS, ROWS), F32),
        in_specs=[SMEM] * RING + [ANY] * len(EARLY) + [VMEM] * RING,
        out_specs=VMEM,
        scratch_shapes=[
            pltpu.VMEM((len(EARLY) * RING * CAP, ROWS, ROWS), BF),
            pltpu.SemaphoreType.DMA((len(EARLY),)),
        ],
        cost_estimate=pl.CostEstimate(flops=10**10, bytes_accessed=2 * 10**7, transcendentals=0),
        compiler_params=grant(15),
        name="early",
    )(*lists, *sources, *nbrs)


def late_kernel(*refs):
    lists, src, nbr = refs[:RING], refs[RING : RING + len(LATE)], refs[RING + len(LATE) : 2 * RING + len(LATE)]
    _, *outs, acc = refs[2 * RING + len(LATE) :]

    def block_of(q, b):
        return jnp.where(q == LATE[0], src[0][b], src[1][b])

    add_sums(lists, nbr, block_of, acc, 1)
    for m in range(RING):

        def leave(n, _, m=m):
            outs[m][n] = acc[m * DST + n].astype(BF)
            return 0

        lax.fori_loop(0, DST, leave, 0, unroll=4)


def late_sums(lists, sources, nbrs, early):
    n_in = 2 * RING + len(LATE)
    return pl.pallas_call(
        late_kernel,
        out_shape=[jax.ShapeDtypeStruct((DST, ROWS, ROWS), BF)] * RING + [jax.ShapeDtypeStruct(early.shape, F32)],
        in_specs=[SMEM] * RING + [VMEM] * (len(LATE) + RING + 1),
        out_specs=[VMEM] * (RING + 1),
        input_output_aliases={n_in: RING},
        cost_estimate=pl.CostEstimate(flops=10**10, bytes_accessed=2 * 10**7, transcendentals=0),
        compiler_params=grant(12),
        name="late",
    )(*lists, *sources, *nbrs, early)[:RING]


def join_own_kernel(a, b, c, d, out):
    for n in range(DST):
        out[n] = (a[n].astype(F32) + b[n].astype(F32) + c[n].astype(F32) + d[n].astype(F32)).astype(BF)


def join_agg_kernel(column, tile_count, a, b, c, d, *outs):
    for k, out in enumerate(outs):
        for j in range(ROW_BLK):
            n = ((column[0] + k) & (N_COL - 1)) * ROW_BLK + j
            total = a[n].astype(F32) + b[n].astype(F32) + c[n].astype(F32) + d[n].astype(F32)
            out[j] = (total / (tile_count[n] * FAN_T).astype(F32)).astype(BF)


def join(kernel, scalars, parts, shapes):
    return pl.pallas_call(
        kernel,
        out_shape=[jax.ShapeDtypeStruct(shape, BF) for shape in shapes],
        in_specs=[SMEM] * len(scalars) + [VMEM] * RING,
        out_specs=[VMEM] * len(shapes),
        cost_estimate=pl.CostEstimate(flops=10**9, bytes_accessed=5 * 10**6, transcendentals=0),
        compiler_params=LIMIT,
    )(*scalars, *parts)


def gather_kernel(*refs):
    *parts, out = refs
    for k, part in enumerate(parts):
        out[k] = part[...]


def gather_weights(parts):
    return pl.pallas_call(
        gather_kernel,
        out_shape=jax.ShapeDtypeStruct((len(parts), *parts[0].shape), BF),
        in_specs=[VMEM] * len(parts),
        out_specs=VMEM,
        cost_estimate=pl.CostEstimate(flops=10**9, bytes_accessed=5 * 10**6, transcendentals=0),
        compiler_params=LIMIT,
        name="gather_weights",
    )(*parts)


def project_kernel(me, column, xs, *refs):
    xa, (w_mine, w_other, out, hid) = refs[:N_COL], refs[N_COL:]
    self_first = me[0] & 1 == 0
    for b in range(ROW_BLK):
        for n0 in range(0, D, 256):
            total = None
            for k in range(N_COL):
                s, a = xs[(column[0] - k) & (N_COL - 1), b], xa[k][b]
                x = jnp.concatenate([jnp.where(self_first, s, a), jnp.where(self_first, a, s)], axis=0)
                w = jnp.concatenate([w_mine[k, n0 : n0 + 256, :], w_other[k, n0 : n0 + 256, :]], axis=1)
                part = jnp.dot(w, x, preferred_element_type=F32)
                total = part if total is None else total + part
            hid[n0 : n0 + 256, :] = jnp.maximum(total, 0.0)
        h = hid[...]
        scale = jnp.sqrt(0.25 + jnp.sum(h * h, axis=0, keepdims=True) / D)
        for j in range(N_COL):
            piece = hid[j * ROWS : (j + 1) * ROWS, :] / scale
            out[j, b * ROWS : (b + 1) * ROWS, :] = piece.T.astype(BF)


def project(me, column, xs, xa, w_mine, w_other):
    return pl.pallas_call(
        project_kernel,
        out_shape=jax.ShapeDtypeStruct((N_COL, ROW_BLK * ROWS, ROWS), BF),
        in_specs=[SMEM] * 2 + [VMEM] * (N_COL + 3),
        out_specs=VMEM,
        scratch_shapes=[pltpu.VMEM((D, ROWS), F32)],
        cost_estimate=pl.CostEstimate(flops=10**9, bytes_accessed=5 * 10**6, transcendentals=0),
        compiler_params=LIMIT,
        name="project",
    )(me, column, xs, *xa, w_mine, w_other)


def body(features, requests, counts, tile_block, local_nbr, tile_count, w_self, w_neigh):
    me = lax.axis_index("dom").reshape(1).astype(I32)
    column = lax.axis_index("col").reshape(1).astype(I32)
    packed = pack(me, requests[0].T, features)
    sources = [packed[0]]
    for q in range(1, N_SRC):
        if q in LATE:
            d = 1 if q % 2 == 0 else RING - 1
            hop = lax.ppermute(packed[q], "dom", meet_pairs(d, q % 2))
            sources.append(lax.ppermute(hop, "dom", meet_pairs(d, 0)))
        else:
            sources.append(lax.ppermute(packed[q], "dom", meet_pairs(q // 2, q % 2)))

    todo = plan(me, counts[:, 0], tile_block, tile_count)
    nbr_t = turn_nbr(local_nbr)
    w_t = turn_weights(me, w_self, w_neigh)
    lists, nbrs = [todo], [nbr_t]
    for m in range(1, RING):
        lists.append(lax.ppermute(todo, "dom", ring_pairs(m)))
        nbrs.append(lax.ppermute(nbr_t, "dom", ring_pairs(m)))
    w_all = [w_t]
    for k in range(1, N_COL):
        w_all.append(lax.ppermute(w_t, "col", col_pairs(k)))
    w_mine = gather_weights(w_all)
    w_other = lax.ppermute(w_mine, "dom", [(i, i ^ 1) for i in range(lax.axis_size("dom"))])

    own_parts = own_rows(lists, sources)
    own_here = [own_parts[0]]
    for m in range(1, RING):
        own_here.append(lax.ppermute(own_parts[m], "dom", ring_pairs(RING - m)))
    early = early_sums(lists, [sources[q] for q in EARLY], nbrs)
    agg_parts = late_sums(lists, [sources[q] for q in LATE], nbrs, early)
    agg_here = [agg_parts[0]]
    for m in range(1, RING):
        agg_here.append(lax.ppermute(agg_parts[m], "dom", ring_pairs(RING - m)))

    (own_sum,) = join(join_own_kernel, (), own_here, [(DST, ROWS, ROWS)])
    xs = lax.all_to_all(own_sum.reshape(N_COL, ROW_BLK, ROWS, ROWS), "col", 0, 0, tiled=True)
    parts = join(join_agg_kernel, (column, tile_count), agg_here, [(ROW_BLK, ROWS, ROWS)] * N_COL)
    xa = [parts[0]] + [lax.ppermute(parts[k], "col", col_pairs(k)) for k in range(1, N_COL)]
    y = project(me, column, xs, xa, w_mine, w_other)
    return lax.all_to_all(y, "col", 0, 0, tiled=True).reshape(-1, ROWS)


def solution(mesh):
    return jax.shard_map(
        body,
        mesh=mesh,
        in_specs=(
            P("dom", "col"),
            P("dom", None, None),
            P(None, "dom"),
            P("dom", None),
            P("dom", None),
            P("dom"),
            P("col", None),
            P("col", None),
        ),
        out_specs=P("dom", "col"),
        check_vma=False,
    )
```

```python
import functools

import jax
import jax.numpy as jnp
from jax import lax
from jax.experimental import pallas as pl
from jax.experimental.pallas import tpu as pltpu
from jax.sharding import PartitionSpec as P


D = 1024
ROWS = 128
CAP = 8
TILES = 32
FAN_T = 4
FRONT = 128
RING = 4
N_SRC = 2 * RING
DST = 16
N_COL = 8
ROW_BLK = DST // N_COL
N_ITEMS = DST * TILES
SECTION = N_ITEMS + ROWS
UNROLL = 4
EARLY = (0, 1, 2, 3, 6, 7)
LATE = (4, 5)
HALVES = ((0, 1), (2, 3))
BF = jnp.bfloat16
F32 = jnp.float32
I32 = jnp.int32

VMEM = pl.BlockSpec(memory_space=pltpu.VMEM)
SMEM = pl.BlockSpec(memory_space=pltpu.SMEM)
ANY = pl.BlockSpec(memory_space=pl.ANY)


def grant(mib):
    return pltpu.CompilerParams(vmem_limit_bytes=mib * 2**20)


LIMIT = grant(8)


def dom_of(y, x, core):
    return (y * RING + x) * 2 + core


def meet_pairs(d, e):
    pairs = []
    for y in range(RING):
        for x in range(RING):
            for core in range(2):
                if core ^ e == 0:
                    pairs.append((dom_of(y, x, core), dom_of((y + d) % RING, x, 0)))
                else:
                    pairs.append((dom_of(y, x, core), dom_of(y, (x + d) % RING, 1)))
    return pairs


def ring_pairs(m):
    pairs = []
    for y in range(RING):
        for x in range(RING):
            pairs.append((dom_of(y, x, 0), dom_of(y, (x + m) % RING, 0)))
            pairs.append((dom_of(y, x, 1), dom_of((y + m) % RING, x, 1)))
    return pairs


def col_pairs(k):
    return [(i, (i + k) % N_COL) for i in range(N_COL)]


def wrapped(v):
    return lax.rem(v + 2 * RING, RING)


def pack_kernel(me, req, feat, *refs):
    outs, (ft, stage, sem) = refs[:N_SRC], refs[N_SRC:]
    core, x, y = lax.rem(me[0], 2), lax.rem(me[0] // 2, RING), me[0] // (2 * RING)

    def turn(b, _):
        for u in range(8):
            ft[b * 8 + u] = feat[pl.ds((b * 8 + u) * ROWS, ROWS), :].T
        return 0

    lax.fori_loop(0, feat.shape[0] // ROWS // 8, turn, 0)
    copies = []
    for q in range(N_SRC):
        d, e = q // 2, q % 2
        to_one = lax.rem(core + e, 2)
        for m in range(RING):
            shard0 = dom_of(wrapped(y + d), wrapped(x - m), 0)
            shard1 = dom_of(wrapped(y - m), wrapped(x + d), 1)
            shard = jnp.where(to_one == 1, shard1, shard0)
            for s in range(CAP):
                stage[q, m * CAP + s] = ft[req[s, shard]]
        copy = pltpu.make_async_copy(stage.at[q], outs[q], sem.at[q])
        copy.start()
        copies.append(copy)
    for copy in copies:
        copy.wait()


def pack(me, requests, features):
    n_blk = features.shape[0] // ROWS
    return pl.pallas_call(
        pack_kernel,
        out_shape=[jax.ShapeDtypeStruct((RING * CAP, ROWS, ROWS), BF)] * N_SRC,
        in_specs=[SMEM, SMEM, VMEM],
        out_specs=[ANY] * N_SRC,
        scratch_shapes=[
            pltpu.VMEM((n_blk, ROWS, ROWS), BF),
            pltpu.VMEM((N_SRC, RING * CAP, ROWS, ROWS), BF),
            pltpu.SemaphoreType.DMA((N_SRC,)),
        ],
        cost_estimate=pl.CostEstimate(flops=10**9, bytes_accessed=10**7, transcendentals=0),
        compiler_params=grant(14),
        name="pack",
    )(me, requests, features)


def turn_nbr_kernel(nbr, out):
    half = ROWS // 2
    for i in range(nbr.shape[0] // ROWS):
        turned = nbr[i * ROWS : (i + 1) * ROWS, :].T
        out[i * half : (i + 1) * half, :] = turned[:half] + turned[half:] * 65536


def turn_nbr(local_nbr):
    some = 4 * ROWS
    return pl.pallas_call(
        turn_nbr_kernel,
        grid=(local_nbr.shape[0] // some,),
        out_shape=jax.ShapeDtypeStruct((local_nbr.shape[0] // 2, ROWS), I32),
        in_specs=[pl.BlockSpec((some, ROWS), lambda g: (g, 0))],
        out_specs=pl.BlockSpec((some // 2, ROWS), lambda g: (g, 0)),
        cost_estimate=pl.CostEstimate(flops=10**9, bytes_accessed=10**7, transcendentals=0),
        compiler_params=LIMIT,
        name="turn_nbr",
    )(local_nbr)


def turn_weights_kernel(me, ws, wn, w_t):
    for core, w in enumerate((ws, wn)):

        @pl.when(me[0] & 1 == core)
        def _():
            for j in range(D // ROWS):
                w_t[j * ROWS : (j + 1) * ROWS, :] = w[:, j * ROWS : (j + 1) * ROWS].T


def turn_weights(me, w_self, w_neigh):
    return pl.pallas_call(
        turn_weights_kernel,
        out_shape=jax.ShapeDtypeStruct((D, ROWS), BF),
        in_specs=[SMEM] + [VMEM] * 2,
        out_specs=VMEM,
        cost_estimate=pl.CostEstimate(flops=10**9, bytes_accessed=10**7, transcendentals=0),
        compiler_params=LIMIT,
        name="turn_weights",
    )(me, w_self, w_neigh)


def plan_kernel(me, cnt, tile_block, tile_count, todo, slot, size):
    core, x, y = me[0] & 1, (me[0] >> 1) & (RING - 1), me[0] >> 3
    for m in range(RING):
        size[m] = m * SECTION
        size[RING + m] = m * SECTION + N_ITEMS - 1
    size[2 * RING] = RING * SECTION + SECTION // 2

    def owner(o, p):
        co, xo, yo = o & 1, (o >> 1) & (RING - 1), o >> 3
        q0 = ((y - yo) & (RING - 1)) * 2 + co
        q1 = ((x - xo) & (RING - 1)) * 2 + 1 - co
        q = jnp.where(core == 0, q0, q1)
        m = jnp.where(core == 0, xo - x, yo - y) & (RING - 1)
        first = q * 32 + m * CAP

        def one(s, p):
            slot[p] = first + s
            return p + 1

        return lax.fori_loop(0, cnt[o], one, p)

    lax.fori_loop(0, 2 * RING * RING, owner, jnp.int32(0))

    def block(i, _):
        v = slot[i]
        for m in range(RING):
            todo[m * SECTION + N_ITEMS + 2 + i] = jnp.where((v >> 3) & (RING - 1) == m, v, -1)
        used = tile_count[i]

        def tile(h, _):
            vs = [slot[tile_block[i, h * UNROLL + u]] for u in range(UNROLL)]
            for u, v in enumerate(vs):
                t = h * UNROLL + u
                late = v >> 6 == 2
                m = jnp.where(late, RING, 0) + ((v >> 3) & (RING - 1))
                m = jnp.where(t < used, m, 2 * RING)
                n = size[m]
                todo[n] = v + 256 * i + 4096 * t
                size[m] = n + jnp.where(late, -1, 1)
            return 0

        lax.fori_loop(0, (used + UNROLL - 1) // UNROLL, tile, 0)
        return 0

    lax.fori_loop(0, DST, block, 0)
    for m in range(RING):
        todo[m * SECTION + N_ITEMS] = size[m] - m * SECTION
        todo[m * SECTION + N_ITEMS + 1] = m * SECTION + N_ITEMS - 1 - size[RING + m]


def plan(me, counts, tile_block, tile_count):
    return pl.pallas_call(
        plan_kernel,
        out_shape=jax.ShapeDtypeStruct(((RING + 1) * SECTION,), I32),
        in_specs=[SMEM] * 4,
        out_specs=SMEM,
        scratch_shapes=[pltpu.SMEM((FRONT,), I32), pltpu.SMEM((2 * RING + 1,), I32)],
        cost_estimate=pl.CostEstimate(flops=2 * 10**9, bytes_accessed=10**6, transcendentals=0),
        compiler_params=LIMIT,
        name="plan",
    )(me, counts, tile_block, tile_count)


def own_kernel(*refs):
    lists, src, outs = refs[:RING], refs[RING : RING + N_SRC], refs[RING + N_SRC :]
    for m in range(RING):

        def place(i, _, m=m):
            v = lists[m][m * SECTION + N_ITEMS + 2 + i]

            @pl.when(v < 0)
            def _():
                outs[m][i] = jnp.zeros((ROWS, ROWS), BF)

            @pl.when(v >= 0)
            def _():
                for q in range(N_SRC):

                    @pl.when(v >> 5 == q)
                    def _():
                        outs[m][i] = src[q][v & 31]

            return 0

        lax.fori_loop(0, DST, place, 0)


def own_rows(lists, sources):
    return pl.pallas_call(
        own_kernel,
        out_shape=[jax.ShapeDtypeStruct((DST, ROWS, ROWS), BF)] * RING,
        in_specs=[SMEM] * RING + [VMEM] * N_SRC,
        out_specs=[VMEM] * RING,
        cost_estimate=pl.CostEstimate(flops=10**9, bytes_accessed=10**7, transcendentals=0),
        compiler_params=grant(12),
        name="own_rows",
    )(*lists, *sources)


def add_sums(shards, lists, nbr, block_of, acc, late):
    iota = lax.broadcasted_iota(I32, (ROWS, ROWS), 0).astype(F32).astype(BF)
    one, zero = jnp.ones((), BF), jnp.zeros((), BF)
    for at, m in enumerate(shards):
        todo = lists[at]
        n_item = todo[m * SECTION + N_ITEMS + late]

        def some(h, _, at=at, m=m, todo=todo, n_item=n_item):
            parts = []
            for u in range(UNROLL):
                n = h * UNROLL + u
                place = m * SECTION + (N_ITEMS - 1 - n if late else n)
                item = jnp.where(n < n_item, todo[place], 128 * late)
                block = block_of((item >> 5) & 7, item & 31)
                i = (item >> 8) & 15
                t = item >> 12
                row0 = i * (ROWS // 2) + (t & 15) * FAN_T
                shift = (t >> 4) * 16
                total = None
                for f in range(FAN_T):
                    row = (nbr[at][pl.ds(row0 + f, 1), :] >> shift) & 65535
                    hit = jnp.where(iota == row.astype(F32).astype(BF), one, zero)
                    total = hit if total is None else total + hit
                dst = jnp.where(n < n_item, at * DST + i, len(shards) * DST)
                parts.append((dst, jnp.dot(block, total, preferred_element_type=F32)))
            for dst, part in parts:
                acc[dst] += part
            return 0

        lax.fori_loop(0, (n_item + UNROLL - 1) // UNROLL, some, 0)


def early_kernel(shards, *refs):
    n = len(shards)
    lists, src, nbr = refs[:n], refs[n : n + len(EARLY)], refs[n + len(EARLY) : 2 * n + len(EARLY)]
    acc, blocks, sem = refs[2 * n + len(EARLY) :]
    some, first = n * CAP, shards[0] * CAP
    copies = [
        pltpu.make_async_copy(src[q].at[pl.ds(first, some)], blocks.at[pl.ds(q * some, some)], sem.at[q])
        for q in range(len(EARLY))
    ]
    for copy in copies:
        copy.start()

    def clear(i, _):
        acc[i] = jnp.zeros((ROWS, ROWS), F32)
        return 0

    lax.fori_loop(0, n * DST + 1, clear, 0)
    for copy in copies:
        copy.wait()

    def block_of(q, b):
        return blocks[jnp.where(q > 3, q - 2, q) * some + jnp.maximum(b - first, 0)]

    add_sums(shards, lists, nbr, block_of, acc, 0)


def early_sums(shards, lists, sources, nbrs):
    n = len(shards)
    return pl.pallas_call(
        functools.partial(early_kernel, shards),
        out_shape=jax.ShapeDtypeStruct((n * DST + 1, ROWS, ROWS), F32),
        in_specs=[SMEM] * n + [ANY] * len(EARLY) + [VMEM] * n,
        out_specs=VMEM,
        scratch_shapes=[
            pltpu.VMEM((len(EARLY) * n * CAP, ROWS, ROWS), BF),
            pltpu.SemaphoreType.DMA((len(EARLY),)),
        ],
        cost_estimate=pl.CostEstimate(flops=5 * 10**9, bytes_accessed=10**7, transcendentals=0),
        compiler_params=grant(10),
    )(*(lists[m] for m in shards), *sources, *(nbrs[m] for m in shards))


def late_kernel(*refs):
    lists, src, nbr = refs[:RING], refs[RING : RING + len(LATE)], refs[RING + len(LATE) : 2 * RING + len(LATE)]
    outs, accs = refs[-RING - len(HALVES) : -len(HALVES)], refs[-len(HALVES) :]

    def block_of(q, b):
        return jnp.where(q == LATE[0], src[0][b], src[1][b])

    for shards, acc in zip(HALVES, accs):
        add_sums(shards, [lists[m] for m in shards], [nbr[m] for m in shards], block_of, acc, 1)
        for at, m in enumerate(shards):

            def leave(n, _, at=at, m=m, acc=acc):
                outs[m][n] = acc[at * DST + n].astype(BF)
                return 0

            lax.fori_loop(0, DST, leave, 0, unroll=4)


def late_sums(lists, sources, nbrs, early):
    n_in = 2 * RING + len(LATE)
    return pl.pallas_call(
        late_kernel,
        out_shape=[jax.ShapeDtypeStruct((DST, ROWS, ROWS), BF)] * RING
        + [jax.ShapeDtypeStruct(e.shape, F32) for e in early],
        in_specs=[SMEM] * RING + [VMEM] * (len(LATE) + RING + len(early)),
        out_specs=[VMEM] * (RING + len(early)),
        input_output_aliases={n_in + h: RING + h for h in range(len(early))},
        cost_estimate=pl.CostEstimate(flops=10**10, bytes_accessed=2 * 10**7, transcendentals=0),
        compiler_params=grant(6),
        name="late",
    )(*lists, *sources, *nbrs, *early)[:RING]


def join_own_kernel(a, b, c, d, out):
    for n in range(DST):
        out[n] = (a[n].astype(F32) + b[n].astype(F32) + c[n].astype(F32) + d[n].astype(F32)).astype(BF)


def join_agg_kernel(column, tile_count, a, b, c, d, *outs):
    for k, out in enumerate(outs):
        for j in range(ROW_BLK):
            n = ((column[0] + k) & (N_COL - 1)) * ROW_BLK + j
            total = a[n].astype(F32) + b[n].astype(F32) + c[n].astype(F32) + d[n].astype(F32)
            out[j] = (total / (tile_count[n] * FAN_T).astype(F32)).astype(BF)


def join(kernel, scalars, parts, shapes):
    return pl.pallas_call(
        kernel,
        out_shape=[jax.ShapeDtypeStruct(shape, BF) for shape in shapes],
        in_specs=[SMEM] * len(scalars) + [VMEM] * RING,
        out_specs=[VMEM] * len(shapes),
        cost_estimate=pl.CostEstimate(flops=10**9, bytes_accessed=5 * 10**6, transcendentals=0),
        compiler_params=LIMIT,
    )(*scalars, *parts)


def gather_kernel(*refs):
    *parts, out = refs
    for k, part in enumerate(parts):
        out[k] = part[...]


def gather_weights(parts):
    return pl.pallas_call(
        gather_kernel,
        out_shape=jax.ShapeDtypeStruct((len(parts), *parts[0].shape), BF),
        in_specs=[VMEM] * len(parts),
        out_specs=VMEM,
        cost_estimate=pl.CostEstimate(flops=10**9, bytes_accessed=5 * 10**6, transcendentals=0),
        compiler_params=LIMIT,
        name="gather_weights",
    )(*parts)


def project_kernel(me, column, xs, *refs):
    xa, (w_mine, w_other, out, hid) = refs[:N_COL], refs[N_COL:]
    self_first = me[0] & 1 == 0
    for b in range(ROW_BLK):
        for n0 in range(0, D, 256):
            total = None
            for k in range(N_COL):
                s, a = xs[(column[0] - k) & (N_COL - 1), b], xa[k][b]
                x = jnp.concatenate([jnp.where(self_first, s, a), jnp.where(self_first, a, s)], axis=0)
                w = jnp.concatenate([w_mine[k, n0 : n0 + 256, :], w_other[k, n0 : n0 + 256, :]], axis=1)
                part = jnp.dot(w, x, preferred_element_type=F32)
                total = part if total is None else total + part
            hid[n0 : n0 + 256, :] = jnp.maximum(total, 0.0)
        h = hid[...]
        scale = jnp.sqrt(0.25 + jnp.sum(h * h, axis=0, keepdims=True) / D)
        for j in range(N_COL):
            piece = hid[j * ROWS : (j + 1) * ROWS, :] / scale
            out[j, b * ROWS : (b + 1) * ROWS, :] = piece.T.astype(BF)


def project(me, column, xs, xa, w_mine, w_other):
    return pl.pallas_call(
        project_kernel,
        out_shape=jax.ShapeDtypeStruct((N_COL, ROW_BLK * ROWS, ROWS), BF),
        in_specs=[SMEM] * 2 + [VMEM] * (N_COL + 3),
        out_specs=VMEM,
        scratch_shapes=[pltpu.VMEM((D, ROWS), F32)],
        cost_estimate=pl.CostEstimate(flops=10**9, bytes_accessed=5 * 10**6, transcendentals=0),
        compiler_params=LIMIT,
        name="project",
    )(me, column, xs, *xa, w_mine, w_other)


def body(features, requests, counts, tile_block, local_nbr, tile_count, w_self, w_neigh):
    me = lax.axis_index("dom").reshape(1).astype(I32)
    column = lax.axis_index("col").reshape(1).astype(I32)
    packed = pack(me, requests[0].T, features)
    sources = [packed[0]]
    for q in range(1, N_SRC):
        if q in LATE:
            d = 1 if q % 2 == 0 else RING - 1
            hop = lax.ppermute(packed[q], "dom", meet_pairs(d, q % 2))
            sources.append(lax.ppermute(hop, "dom", meet_pairs(d, 0)))
        else:
            sources.append(lax.ppermute(packed[q], "dom", meet_pairs(q // 2, q % 2)))

    todo = plan(me, counts[:, 0], tile_block, tile_count)
    nbr_t = turn_nbr(local_nbr)
    w_t = turn_weights(me, w_self, w_neigh)
    lists, nbrs = [todo], [nbr_t]
    for m in range(1, RING):
        lists.append(lax.ppermute(todo, "dom", ring_pairs(m)))
        nbrs.append(lax.ppermute(nbr_t, "dom", ring_pairs(m)))
    w_all = [w_t]
    for k in range(1, N_COL):
        w_all.append(lax.ppermute(w_t, "col", col_pairs(k)))
    w_mine = gather_weights(w_all)
    w_other = lax.ppermute(w_mine, "dom", [(i, i ^ 1) for i in range(lax.axis_size("dom"))])

    own_parts = own_rows(lists, sources)
    own_here = [own_parts[0]]
    for m in range(1, RING):
        own_here.append(lax.ppermute(own_parts[m], "dom", ring_pairs(RING - m)))
    early = [early_sums(shards, lists, [sources[q] for q in EARLY], nbrs) for shards in HALVES]
    agg_parts = late_sums(lists, [sources[q] for q in LATE], nbrs, early)
    agg_here = [agg_parts[0]]
    for m in range(1, RING):
        agg_here.append(lax.ppermute(agg_parts[m], "dom", ring_pairs(RING - m)))

    (own_sum,) = join(join_own_kernel, (), own_here, [(DST, ROWS, ROWS)])
    xs = lax.all_to_all(own_sum.reshape(N_COL, ROW_BLK, ROWS, ROWS), "col", 0, 0, tiled=True)
    parts = join(join_agg_kernel, (column, tile_count), agg_here, [(ROW_BLK, ROWS, ROWS)] * N_COL)
    xa = [parts[0]] + [lax.ppermute(parts[k], "col", col_pairs(k)) for k in range(1, N_COL)]
    y = project(me, column, xs, xa, w_mine, w_other)
    return lax.all_to_all(y, "col", 0, 0, tiled=True).reshape(-1, ROWS)


def solution(mesh):
    return jax.shard_map(
        body,
        mesh=mesh,
        in_specs=(
            P("dom", "col"),
            P("dom", None, None),
            P(None, "dom"),
            P("dom", None),
            P("dom", None),
            P("dom"),
            P("col", None),
            P("col", None),
        ),
        out_specs=P("dom", "col"),
        check_vma=False,
    )
```
